32 devices in a mesh: fsdp: 4 (over y, x), expert: 8 (over z, core).
Axes of the slice: x: 2, y: 2, z: 4, core: 2. Of those that a mesh axis runs over, the one named last changes fastest.
Arguments:
- tokens: bfloat16 [8192, 2048], P(('fsdp', 'expert')), may hold values from -6 to 6
- segments: int32 [32, 256], P(('fsdp', 'expert')), may hold values from 0 to 7, never falling along the last dimension, each value on 1 to 128 neighbouring positions
- routes: int32 [8192, 8], P(('fsdp', 'expert')), may hold values from 0 to 31, all different within a row; in each aligned block of 256 rows (0 to 255, 256 to 511, ...) at most 80 rows name the same one
- attn_gain: bfloat16 [2048], P('expert'), may hold values from 0.5 to 1.5
- w_query: bfloat16 [2048, 4096], P('expert', 'fsdp'), may hold values from -0.125 to 0.125
- key_matrix: bfloat16 [2048, 512], P('expert', 'fsdp'), may hold values from -0.125 to 0.125
- value_matrix: bfloat16 [2048, 512], P('expert', 'fsdp'), may hold values from -0.125 to 0.125
- output_matrix: bfloat16 [4096, 2048], P(('fsdp', 'expert')), may hold values from -0.25 to 0.25
- query_gain: bfloat16 [128], replicated, may hold values from 0.6 to 4
- key_gain: bfloat16 [128], replicated, may hold values from 0.6 to 4
- ffn_gain: bfloat16 [2048], P('expert'), may hold values from 0.5 to 1.5
- w_router: bfloat16 [2048, 32], P('expert'), may hold values from -0.0625 to 0.0625
- w_gate: bfloat16 [32, 2048, 768], P(('fsdp', 'expert')), may hold values from -0.125 to 0.125
- w_up: bfloat16 [32, 2048, 768], P(('fsdp', 'expert')), may hold values from -0.125 to 0.125
- w_down: bfloat16 [32, 768, 2048], P(('fsdp', 'expert')), may hold values from -0.625 to 0.625
- cotangent: bfloat16 [8192, 2048], P(('fsdp', 'expert')), may hold values from -6 to 6
Outputs:
- output: bfloat16 [8192, 2048], P(('fsdp', 'expert'))
- token_grad: float32 [8192, 2048], P(('fsdp', 'expert'))
- attn_gain_grad: float32 [2048], P('expert')
- query_weight_grad: float32 [2048, 4096], P('expert', 'fsdp')
- key_weight_grad: float32 [2048, 512], P('expert', 'fsdp')
- value_weight_grad: float32 [2048, 512], P('expert', 'fsdp')
- out_weight_grad: float32 [4096, 2048], P(('fsdp', 'expert'))
- query_gain_grad: float32 [128], replicated
- key_gain_grad: float32 [128], replicated
- ffn_gain_grad: float32 [2048], P('expert')
- router_grad: float32 [2048, 32], P('expert')
- gate_grad: float32 [32, 2048, 768], P(('fsdp', 'expert'))
- up_grad: float32 [32, 2048, 768], P(('fsdp', 'expert'))
- down_grad: float32 [32, 768, 2048], P(('fsdp', 'expert'))
The draws below stay inside these ranges and needn't reach their ends.
Inputs may be any that keep to these rules, and one draw needn't show every extreme that they name: `routes`: each token names 8 different experts. Among the 256 tokens of one device no expert is named more than 80 times, a bound that some block reaches. `segments`: within a row the ids never fall; a document holds at most 128 positions.
All inputs are finite; a program needn't handle non-finite values.
Results may differ from the reference program's by a relative error of at most 0.02.
The reference program's roundings to bfloat16 on the way count: a program that leaves them out, or rounds other values in their place, can miss the bound.
Values may be sent and summed in bfloat16 or wider, within the bound.
A program may use at most 384 MiB of HBM per device.

```python
import math
import jax
import jax.numpy as jnp
import numpy as np
from jax import lax

MODEL_WIDTH = 2048
QUERY_HEADS = 32
KEY_VALUE_HEADS = 4
HEAD_SIZE = 128
FF = 768
TOP = 8
SEQ = 256
TOK_DEV = 256
EXPERTS = 32
TOKENS = 8192
CAP = 80


def head_gain(key, salt):
    sub = jax.random.fold_in(key, salt)
    value_rows = jax.random.uniform(sub, (HEAD_SIZE,), jnp.float32, 0.6, 1.6)
    return value_rows.astype(jnp.bfloat16)


def draw_query_gain(key, part):
    return head_gain(key, 11)


def draw_key_gain(key, part):
    return head_gain(key, 23)


def strengthened(drawn, stream_key, source, target, shards_of, factor):
    def block_of(dim):
        return (jnp.arange(drawn.shape[dim]) // (drawn.shape[dim] // shards_of)).reshape((-1,) + (1,) * (drawn.ndim - 1 - dim))

    one_side = jax.random.permutation(stream_key, shards_of)[block_of(target)]
    second = (block_of(target) + shards_of // 2) % shards_of
    return jnp.where((block_of(source) == one_side) | (block_of(source) == second), factor * drawn, drawn)


def shard_levels(rng, extent, shards, least, top_value):
    loudness = 1.0
    for dim, blocks in shards:
        heights = jax.random.uniform(jax.random.fold_in(jax.random.fold_in(rng, 6), dim), (blocks,), jnp.float32, least / len(shards), top_value / len(shards))
        loudness = loudness * jnp.repeat(jnp.exp(heights), extent[dim] // blocks).reshape((-1,) + (1,) * (len(extent) - 1 - dim))
    return loudness


def length_profile(number_of, total, limit, skew):
    portions = [(1 << 20) // math.isqrt(grade ** skew) + 1 for grade in range(2, number_of + 1)]
    surplus, counts = total - limit - (number_of - 1), [1] * (number_of - 1)
    while surplus > 0:
        movable = [i for i in range(number_of - 1) if counts[i] < limit]
        mass, left = sum([portions[i] for i in movable]), surplus
        for i in movable:
            more = min(limit - counts[i], max(1, left * portions[i] // mass), surplus)
            counts[i] = counts[i] + more
            surplus = surplus - more
    return np.array([limit] + counts)


def uneven(stream_key, number_of, total, limit, skew):
    if number_of == 2:
        one = jax.random.randint(stream_key, (), max(1, total - limit), min(limit, total - 1) + 1)
        return jnp.stack([one, total - one])
    lengths = jnp.asarray(length_profile(number_of, total, limit, skew), jnp.int32)
    couples = (number_of - 1) // 2
    giver, taker = lengths[1:1 + 2 * couples:2], lengths[2:2 + 2 * couples:2]
    room = jnp.minimum(giver - 1, limit - taker)
    shifted = jax.random.randint(jax.random.fold_in(stream_key, 1), (couples,), 0, 1 << 20) % (room + 1)
    lengths = lengths.at[1:1 + 2 * couples:2].set(giver - shifted).at[2:2 + 2 * couples:2].set(taker + shifted)
    return lengths[jax.random.permutation(jax.random.fold_in(stream_key, 2), number_of)]


def assign_block(rng, own, number, rows, amount, top, most, skew):
    sequence = jax.random.permutation(rng, amount)
    crowded, common = load_shares(amount, rows * top, most, skew, True), load_shares(amount, rows * top, most, skew, False)
    places = jnp.arange(amount)

    def named(lengths, rotation):
        used = int((lengths > 0).sum())
        fixed = max(1, used // 4)
        passed = fixed + (places - fixed + rotation * (used - fixed)) % max(1, amount - fixed)
        return jnp.zeros((amount,), jnp.int32).at[sequence[jnp.where(places < fixed, places, passed)]].set(jnp.asarray(lengths, jnp.int32))

    lengths = jnp.where(number % 4 == 0, named(crowded, number // 4), named(common, number - number // 4 - 1))
    mixed = jax.random.permutation(jax.random.fold_in(own, 3), amount)
    source_of, sink = mixed[0:amount // 2 * 2:2], mixed[1:amount // 2 * 2:2]
    room = jnp.minimum(lengths[source_of] - 1, most - lengths[sink]) // 2
    room = jnp.where((source_of == sequence[0]) | (sink == sequence[0]) | (lengths[sink] == 0), 0, jnp.maximum(room, 0))
    passed = jax.random.randint(jax.random.fold_in(own, 4), (amount // 2,), 0, 1 << 20) % (room + 1)
    lengths = lengths.at[source_of].add(-passed).at[sink].add(passed)
    items = jnp.searchsorted(jnp.cumsum(lengths), jnp.arange(rows * top), side="right").astype(jnp.int32)
    table = items.reshape(top, rows).T
    table = table[jax.random.permutation(jax.random.fold_in(own, 1), rows)]
    rotation = jax.random.randint(jax.random.fold_in(own, 2), (rows, 1), 0, top)
    return jnp.take_along_axis(table, (jnp.arange(top)[None, :] + rotation) % top, axis=1)


def load_shares(amount, total, bound, skew, full):
    portions = [(1 << 20) // math.isqrt(rank ** skew) + 1 for rank in range(1, amount + 1)]
    largest = bound if full else min(bound, max(-(-total // amount), total * portions[0] // sum(portions)))
    least = 1 if total - largest >= amount - 1 else 0
    holding, rest = [largest] + [least] * (amount - 1), total - largest - least * (amount - 1)
    while rest > 0:
        free = [i for i in range(1, amount) if holding[i] < largest] or [i for i in range(1, amount) if holding[i] < bound]
        pool, budget = sum([portions[i] for i in free]), rest
        for i in free:
            extra = min(bound - holding[i], max(1, budget * portions[i] // pool), rest)
            holding[i] = holding[i] + extra
            rest = rest - extra
    return np.array(holding)


def centred(key, shape, deviation, most, split=(), held_as=jnp.bfloat16):
    drawn = deviation * jax.random.normal(key, shape, jnp.float32)
    if split:
        drawn = drawn * shard_levels(key, shape, split, -0.22, 0.18)
    return jnp.clip(drawn, -most, most).astype(held_as)


def bell_draw_with(stream_key, shape, spread, limit, pieces, heavy, held_as=jnp.bfloat16):
    entries = spread * jax.random.normal(stream_key, shape, jnp.float32)
    if pieces:
        entries = entries * shard_levels(stream_key, shape, pieces, -0.22, 0.18)
    return jnp.clip(strengthened(entries, jax.random.fold_in(stream_key, 3), *heavy), -limit, limit).astype(held_as)


def setup_inputs(seed: int = 0) -> dict:
    seeds = jax.random.split(jax.random.key(seed), 17)
    tokens = bell_draw_with(seeds[0], (TOKENS, MODEL_WIDTH), 1.0, 6.0, ((0, 32),), (0, 1, 32, 2.75))
    segments = jax.vmap(lambda own: jnp.searchsorted(jnp.cumsum(uneven(own, 8, SEQ, SEQ // 2, 2)), jnp.arange(SEQ), side="right"))(jax.random.split(seeds[1], (TOKENS // SEQ))).reshape((TOKENS // SEQ, SEQ)).astype(jnp.int32)
    routes_keys = jax.random.split(jax.random.fold_in(seeds[2], 1), TOKENS // TOK_DEV)
    routes_turns = jax.random.permutation(jax.random.fold_in(seeds[2], 3), TOKENS // TOK_DEV)
    routes = jax.vmap(lambda own, number: assign_block(jax.random.fold_in(seeds[2], 2), own, number, TOK_DEV, EXPERTS, TOP, CAP, 2))(routes_keys, routes_turns).reshape((TOKENS, TOP))
    attn_gain = jnp.clip(1.0 + 0.1 * jax.random.normal(seeds[3], (MODEL_WIDTH,), jnp.float32), 0.5, 1.5).astype(jnp.bfloat16)
    w_query = centred(seeds[4], (MODEL_WIDTH, QUERY_HEADS * HEAD_SIZE), MODEL_WIDTH ** -0.5, 0.125, ((0, 8), (1, 4)))
    key_matrix = centred(seeds[5], (MODEL_WIDTH, KEY_VALUE_HEADS * HEAD_SIZE), MODEL_WIDTH ** -0.5, 0.125, ((0, 8), (1, 4)))
    value_matrix = centred(seeds[6], (MODEL_WIDTH, KEY_VALUE_HEADS * HEAD_SIZE), MODEL_WIDTH ** -0.5, 0.125, ((0, 8), (1, 4)))
    output_matrix = centred(seeds[7], (QUERY_HEADS * HEAD_SIZE, MODEL_WIDTH), (QUERY_HEADS * HEAD_SIZE // 8) ** -0.5, 0.25, ((0, 32),))
    query_gain = draw_query_gain(jax.random.fold_in(seeds[16], 71), 0)
    key_gain = draw_key_gain(jax.random.fold_in(seeds[16], 71), 0)
    ffn_gain = jnp.clip(1.0 + 0.1 * jax.random.normal(seeds[10], (MODEL_WIDTH,), jnp.float32), 0.5, 1.5).astype(jnp.bfloat16)
    w_router = centred(seeds[11], (MODEL_WIDTH, EXPERTS), (4 * MODEL_WIDTH) ** -0.5, 0.0625, ((0, 8),))
    w_gate = centred(seeds[12], (EXPERTS, MODEL_WIDTH, FF), MODEL_WIDTH ** -0.5, 0.125, ((0, 32),))
    w_up = centred(seeds[13], (EXPERTS, MODEL_WIDTH, FF), MODEL_WIDTH ** -0.5, 0.125, ((0, 32),))
    w_down = centred(seeds[14], (EXPERTS, FF, MODEL_WIDTH), (FF // 8) ** -0.5, 0.625, ((0, 32),))
    cotangent = centred(seeds[15], (TOKENS, MODEL_WIDTH), 1.0, 6.0, ((0, 32),))
    return {"tokens": tokens, "segments": segments, "routes": routes, "attn_gain": attn_gain, "w_query": w_query, "key_matrix": key_matrix, "value_matrix": value_matrix, "output_matrix": output_matrix, "query_gain": query_gain, "key_gain": key_gain, "ffn_gain": ffn_gain, "w_router": w_router, "w_gate": w_gate, "w_up": w_up, "w_down": w_down, "cotangent": cotangent}


EPS = 1e-06
THETA = 1000000.0
NEG = -1e+30

def inverse_norm(value):
    return lax.rsqrt(lax.optimization_barrier(jnp.mean(value * value, axis=-1, keepdims=True)) + EPS)

def rotary_tables(sequence_length, width):
    half = width // 2
    inverse = THETA ** (-(jnp.arange(half).astype(jnp.float32) * 2.0 / width))
    angle = jnp.arange(sequence_length).astype(jnp.float32)[:, None] * inverse[None, :]
    return (jnp.cos(angle)[None, :, None, :], jnp.sin(angle)[None, :, None, :])

def rotate(value, cosine, sine):
    half = value.shape[-1] // 2
    first = value[..., :half]
    second = value[..., half:]
    return jnp.concatenate([first * cosine - second * sine, second * cosine + first * sine], axis=-1)

def rotate_back(grad, cosine, sine):
    half = grad.shape[-1] // 2
    first = grad[..., :half]
    second = grad[..., half:]
    return jnp.concatenate([first * cosine + second * sine, second * cosine - first * sine], axis=-1)

def attention_parts(block_in, segs, w_query, key_matrix, value_matrix, attn_gain, query_gain, key_gain):
    batch_size, sequence_length, width = block_in.shape
    wide_in = block_in.astype(jnp.float32).reshape(batch_size * sequence_length, width)
    rinv_one = inverse_norm(wide_in)
    first_normed_rows = (wide_in * rinv_one * attn_gain.astype(jnp.float32)).astype(jnp.bfloat16)
    query = jnp.dot(first_normed_rows, w_query, preferred_element_type=jnp.float32).reshape(batch_size, sequence_length, QUERY_HEADS, HEAD_SIZE)
    key_rows = jnp.dot(first_normed_rows, key_matrix, preferred_element_type=jnp.float32).reshape(batch_size, sequence_length, KEY_VALUE_HEADS, HEAD_SIZE)
    value_rows = jnp.dot(first_normed_rows, value_matrix, preferred_element_type=jnp.float32).astype(jnp.bfloat16).reshape(batch_size, sequence_length, KEY_VALUE_HEADS, HEAD_SIZE)
    q_rinv = inverse_norm(query)
    k_rinv = inverse_norm(key_rows)
    cosine, sine = rotary_tables(sequence_length, HEAD_SIZE)
    query_rotated = rotate(query * q_rinv * query_gain.astype(jnp.float32), cosine, sine).astype(jnp.bfloat16)
    k_rot = rotate(key_rows * k_rinv * key_gain.astype(jnp.float32), cosine, sine).astype(jnp.bfloat16)
    grouped_rows = query_rotated.reshape(batch_size, sequence_length, KEY_VALUE_HEADS, QUERY_HEADS // KEY_VALUE_HEADS, HEAD_SIZE)
    scores = jnp.einsum('bqkgd,bskd->bkgqs', grouped_rows.astype(jnp.float32), k_rot.astype(jnp.float32)) * HEAD_SIZE ** (-0.5)
    later = jnp.arange(sequence_length)[:, None] >= jnp.arange(sequence_length)[None, :]
    allowed = (segs[:, :, None] == segs[:, None, :]) & later[None]
    masked = jnp.where(allowed[:, None, None], scores, NEG)
    top = lax.optimization_barrier(jnp.max(masked, axis=-1, keepdims=True))
    lse = top + jnp.log(lax.optimization_barrier(jnp.sum(jnp.exp(masked - top), axis=-1, keepdims=True)))
    prob = jnp.exp(masked - lse)
    prob_low = prob.astype(jnp.bfloat16)
    mixed = jnp.einsum('bkgqs,bskd->bqkgd', prob_low.astype(jnp.float32), value_rows.astype(jnp.float32)).astype(jnp.bfloat16)
    return (wide_in, rinv_one, first_normed_rows, query, q_rinv, key_rows, k_rinv, value_rows, query_rotated, k_rot, prob, prob_low, mixed, cosine, sine)

def head_norm_back(grad_rot, raw, rinv, gain, cosine, sine):
    grad_normed = rotate_back(grad_rot, cosine, sine)
    gain_grad = lax.optimization_barrier(jnp.sum(grad_normed * raw * rinv, axis=(0, 1, 2)))
    scaled = grad_normed * gain
    grad_raw = rinv * scaled - raw * rinv ** 3 * lax.optimization_barrier(jnp.mean(scaled * raw, axis=-1, keepdims=True))
    return (grad_raw, gain_grad)

def row_norm_back(grad_normed, raw, rinv, gain):
    gain_grad = lax.optimization_barrier(jnp.sum(grad_normed * raw * rinv, axis=0))
    scaled = grad_normed * gain
    grad_raw = rinv * scaled - raw * rinv ** 3 * lax.optimization_barrier(jnp.mean(scaled * raw, axis=-1, keepdims=True))
    return (grad_raw, gain_grad)

def attention_backward(block_in, segs, d_mid, w_query, key_matrix, value_matrix, output_matrix, attn_gain, query_gain, key_gain):
    batch_size, sequence_length, width = block_in.shape
    query_groups = QUERY_HEADS // KEY_VALUE_HEADS
    scale = HEAD_SIZE ** (-0.5)
    parts = attention_parts(block_in, segs, w_query, key_matrix, value_matrix, attn_gain, query_gain, key_gain)
    wide_in, rinv_one, first_normed_rows, query, q_rinv, key_rows, k_rinv, value_rows, query_rotated, k_rot, prob, prob_low, mixed, cosine, sine = parts
    mixed_flat = mixed.reshape(batch_size * sequence_length, QUERY_HEADS * HEAD_SIZE)
    middle_grad_narrow = d_mid.astype(jnp.bfloat16)
    out_grad = jnp.dot(mixed_flat.T, middle_grad_narrow, preferred_element_type=jnp.float32)
    mixed_rows_grad = jnp.dot(middle_grad_narrow, output_matrix.T, preferred_element_type=jnp.float32).astype(jnp.bfloat16).reshape(batch_size, sequence_length, KEY_VALUE_HEADS, query_groups, HEAD_SIZE)
    value_rows_grad = jnp.einsum('bkgqs,bqkgd->bskd', prob_low.astype(jnp.float32), mixed_rows_grad.astype(jnp.float32))
    d_prob = jnp.einsum('bqkgd,bskd->bkgqs', mixed_rows_grad.astype(jnp.float32), value_rows.astype(jnp.float32))
    delta = lax.optimization_barrier(jnp.sum(mixed_rows_grad.astype(jnp.float32) * mixed.astype(jnp.float32), axis=-1))
    delta = jnp.transpose(delta, (0, 2, 3, 1))[..., None]
    d_scores = (prob * (d_prob - delta)).astype(jnp.bfloat16)
    grouped_rows = query_rotated.reshape(batch_size, sequence_length, KEY_VALUE_HEADS, query_groups, HEAD_SIZE)
    d_qrot = jnp.einsum('bkgqs,bskd->bqkgd', d_scores.astype(jnp.float32), k_rot.astype(jnp.float32)).reshape(batch_size, sequence_length, QUERY_HEADS, HEAD_SIZE) * scale
    d_krot = jnp.einsum('bkgqs,bqkgd->bskd', d_scores.astype(jnp.float32), grouped_rows.astype(jnp.float32)) * scale
    d_query, q_gain_grad = head_norm_back(d_qrot, query, q_rinv, query_gain.astype(jnp.float32), cosine, sine)
    key_rows_grad, k_gain_grad = head_norm_back(d_krot, key_rows, k_rinv, key_gain.astype(jnp.float32), cosine, sine)
    dq_low = d_query.astype(jnp.bfloat16).reshape(batch_size * sequence_length, QUERY_HEADS * HEAD_SIZE)
    key_grad_narrow = key_rows_grad.astype(jnp.bfloat16).reshape(batch_size * sequence_length, KEY_VALUE_HEADS * HEAD_SIZE)
    value_grad_narrow = value_rows_grad.astype(jnp.bfloat16).reshape(batch_size * sequence_length, KEY_VALUE_HEADS * HEAD_SIZE)
    query_grad = jnp.dot(first_normed_rows.T, dq_low, preferred_element_type=jnp.float32)
    key_grad = jnp.dot(first_normed_rows.T, key_grad_narrow, preferred_element_type=jnp.float32)
    value_grad = jnp.dot(first_normed_rows.T, value_grad_narrow, preferred_element_type=jnp.float32)
    d_normed_one = jnp.dot(dq_low, w_query.T, preferred_element_type=jnp.float32)
    d_normed_one = d_normed_one + jnp.dot(key_grad_narrow, key_matrix.T, preferred_element_type=jnp.float32)
    d_normed_one = d_normed_one + jnp.dot(value_grad_narrow, value_matrix.T, preferred_element_type=jnp.float32)
    d_tokens, gain_grad = row_norm_back(d_normed_one, wide_in, rinv_one, attn_gain.astype(jnp.float32))
    return (d_mid + d_tokens, (gain_grad, query_grad, key_grad, value_grad, out_grad, q_gain_grad, k_gain_grad))

def reference(tokens, segments, routes, attn_gain, w_query, key_matrix, value_matrix, output_matrix, query_gain, key_gain, ffn_gain, w_router, w_gate, w_up, w_down, cotangent):
    nseq = TOKENS // SEQ
    per = math.gcd(nseq, max(1, 4096 // SEQ))
    nblocks = nseq // per
    block_in = tokens.reshape(nblocks, per, SEQ, MODEL_WIDTH)
    block_seg = segments.reshape(nblocks, per, SEQ)

    def forward_block(inputs):
        xin, segs = inputs
        parts = attention_parts(xin, segs, w_query, key_matrix, value_matrix, attn_gain, query_gain, key_gain)
        mixed_flat = parts[12].reshape(per * SEQ, QUERY_HEADS * HEAD_SIZE)
        return parts[0] + jnp.dot(mixed_flat, output_matrix, preferred_element_type=jnp.float32)
    residual_mid = lax.map(forward_block, (block_in, block_seg)).reshape(TOKENS, MODEL_WIDTH)
    rinv_two = inverse_norm(residual_mid)
    gain_two = ffn_gain.astype(jnp.float32)
    normed_two = (residual_mid * rinv_two * gain_two).astype(jnp.bfloat16)
    logits = jnp.dot(normed_two, w_router, preferred_element_type=jnp.float32)
    chosen = jnp.take_along_axis(logits, routes, axis=1)
    top = lax.optimization_barrier(jnp.max(chosen, axis=-1, keepdims=True))
    raised = jnp.exp(chosen - top)
    gates = raised / lax.optimization_barrier(jnp.sum(raised, axis=-1, keepdims=True))
    gates_flat = gates.reshape(-1)
    assign = TOKENS * TOP
    per_device = TOK_DEV * TOP

    def rank_of(row):
        hot = (row[:, None] == jnp.arange(EXPERTS)[None, :]).astype(jnp.int32)
        return lax.optimization_barrier(jnp.sum(hot * jnp.cumsum(hot, axis=0), axis=1)) - 1
    ranks = lax.map(rank_of, routes.reshape(EXPERTS, per_device)).reshape(-1).astype(jnp.int32)
    device_of = (jnp.arange(assign) // per_device).astype(jnp.int32)
    width_e = EXPERTS * CAP
    place = routes.reshape(-1).astype(jnp.int32) * width_e + device_of * CAP + ranks
    table = jnp.zeros((EXPERTS * width_e,), jnp.int32).at[place].set(jnp.arange(assign).astype(jnp.int32) + 1)
    table = table.reshape(EXPERTS, width_e)
    upstream = cotangent.astype(jnp.float32)

    def expert_step(carry, inputs):
        moe, d_normed_two, d_gates = carry
        entry, gate_w, up_w, down_w = inputs
        filled = entry > 0
        which = jnp.maximum(entry - 1, 0)
        token_of = which // TOP
        rows = jnp.where(filled[:, None], normed_two[token_of], jnp.zeros((), jnp.bfloat16))
        gate_pre = jnp.dot(rows, gate_w, preferred_element_type=jnp.float32)
        up_pre = jnp.dot(rows, up_w, preferred_element_type=jnp.float32)
        sigma = jax.nn.sigmoid(gate_pre)
        act = (gate_pre * sigma * up_pre).astype(jnp.bfloat16)
        expert_out = jnp.dot(act, down_w, preferred_element_type=jnp.float32).astype(jnp.bfloat16)
        out_wide = expert_out.astype(jnp.float32)
        weight = jnp.where(filled, gates_flat[which], 0.0)
        moe = moe.at[token_of].add(weight[:, None] * out_wide)
        dy_rows = upstream[token_of]
        d_gates = d_gates.at[which].add(jnp.where(filled, lax.optimization_barrier(jnp.sum(dy_rows * out_wide, axis=-1)), 0.0))
        d_expert = (weight[:, None] * dy_rows).astype(jnp.bfloat16)
        d_act = jnp.dot(d_expert, down_w.T, preferred_element_type=jnp.float32)
        down_grad = jnp.dot(act.T, d_expert, preferred_element_type=jnp.float32)
        d_gate_pre = (d_act * up_pre * sigma * (1.0 + gate_pre * (1.0 - sigma))).astype(jnp.bfloat16)
        d_up_pre = (d_act * gate_pre * sigma).astype(jnp.bfloat16)
        gate_grad = jnp.dot(rows.T, d_gate_pre, preferred_element_type=jnp.float32)
        up_grad = jnp.dot(rows.T, d_up_pre, preferred_element_type=jnp.float32)
        d_rows = jnp.dot(d_gate_pre, gate_w.T, preferred_element_type=jnp.float32)
        d_rows = (d_rows + jnp.dot(d_up_pre, up_w.T, preferred_element_type=jnp.float32)).astype(jnp.bfloat16)
        d_normed_two = d_normed_two.at[token_of].add(jnp.where(filled[:, None], d_rows.astype(jnp.float32), 0.0))
        return ((moe, d_normed_two, d_gates), (gate_grad, up_grad, down_grad))
    start = (jnp.zeros((TOKENS, MODEL_WIDTH), jnp.float32), jnp.zeros((TOKENS, MODEL_WIDTH), jnp.float32), jnp.zeros((assign,), jnp.float32))
    (moe, d_normed_two, d_gates), (gate_grad, up_grad, down_grad) = lax.scan(expert_step, start, (table, w_gate, w_up, w_down))
    output = (residual_mid + moe).astype(jnp.bfloat16)
    d_gates = d_gates.reshape(TOKENS, TOP)
    d_chosen = gates * (d_gates - lax.optimization_barrier(jnp.sum(gates * d_gates, axis=-1, keepdims=True)))
    hot = (routes[:, :, None] == jnp.arange(EXPERTS)[None, None, :]).astype(jnp.float32)
    d_logits = lax.optimization_barrier(jnp.sum(hot * d_chosen[:, :, None], axis=1)).astype(jnp.bfloat16)
    router_grad = jnp.dot(normed_two.T, d_logits, preferred_element_type=jnp.float32)
    d_normed_two = d_normed_two + jnp.dot(d_logits, w_router.T, preferred_element_type=jnp.float32)
    d_norm_part, ffn_gain_grad = row_norm_back(d_normed_two, residual_mid, rinv_two, gain_two)
    d_mid = upstream + d_norm_part

    def backward_step(total, inputs):
        xin, segs, grad_mid = inputs
        d_tokens, grads = attention_backward(xin, segs, grad_mid, w_query, key_matrix, value_matrix, output_matrix, attn_gain, query_gain, key_gain)
        return (jax.tree.map(jnp.add, total, grads), d_tokens)
    empty_gradients = (jnp.zeros((MODEL_WIDTH,), jnp.float32), jnp.zeros((MODEL_WIDTH, QUERY_HEADS * HEAD_SIZE), jnp.float32), jnp.zeros((MODEL_WIDTH, KEY_VALUE_HEADS * HEAD_SIZE), jnp.float32), jnp.zeros((MODEL_WIDTH, KEY_VALUE_HEADS * HEAD_SIZE), jnp.float32), jnp.zeros((QUERY_HEADS * HEAD_SIZE, MODEL_WIDTH), jnp.float32), jnp.zeros((HEAD_SIZE,), jnp.float32), jnp.zeros((HEAD_SIZE,), jnp.float32))
    sums, d_tokens = lax.scan(backward_step, empty_gradients, (block_in, block_seg, d_mid.reshape(nblocks, per * SEQ, MODEL_WIDTH)))
    gain_grad, query_grad, key_grad, value_grad, out_grad, q_gain_grad, k_gain_grad = sums
    token_grad = d_tokens.reshape(TOKENS, MODEL_WIDTH)
    return (output, token_grad, gain_grad, query_grad, key_grad, value_grad, out_grad, q_gain_grad, k_gain_grad, ffn_gain_grad, router_grad, gate_grad, up_grad, down_grad)
```

```python
import jax
import jax.numpy as jnp
from jax import lax
from jax.experimental import pallas as pl
from jax.experimental.pallas import tpu as pltpu
from jax.sharding import PartitionSpec as P

MODEL_WIDTH = 2048
HEAD_SIZE = 128
TOP = 8
SEQ = 256


EPS = 1e-06
THETA = 1000000.0
NEG = -1e30


def inverse_norm(value):
    return lax.rsqrt(jnp.mean(value * value, axis=-1, keepdims=True) + EPS)


def rotary_tables(sequence_length, width):
    half = width // 2
    inverse = THETA ** (-(jnp.arange(half).astype(jnp.float32) * 2.0 / width))
    angle = jnp.arange(sequence_length).astype(jnp.float32)[:, None] * inverse[None, :]
    return (jnp.cos(angle)[None, :, None, :], jnp.sin(angle)[None, :, None, :])


def rotate(value, cosine, sine):
    half = value.shape[-1] // 2
    first = value[..., :half]
    second = value[..., half:]
    return jnp.concatenate(
        [first * cosine - second * sine, second * cosine + first * sine], axis=-1
    )


def rotate_back(grad, cosine, sine):
    half = grad.shape[-1] // 2
    first = grad[..., :half]
    second = grad[..., half:]
    return jnp.concatenate(
        [first * cosine + second * sine, second * cosine - first * sine], axis=-1
    )


def masked_scores(query_rotated, k_rot, segs):
    batch_size, sequence_length = segs.shape
    kv_heads = k_rot.shape[2]
    grouped_rows = query_rotated.reshape(
        batch_size, sequence_length, kv_heads, query_rotated.shape[2] // kv_heads, HEAD_SIZE
    )
    scores = jnp.einsum(
        "bqkgd,bskd->bkgqs", grouped_rows, k_rot, preferred_element_type=jnp.float32
    ) * HEAD_SIZE ** (-0.5)
    later = jnp.arange(sequence_length)[:, None] >= jnp.arange(sequence_length)[None, :]
    allowed = (segs[:, :, None] == segs[:, None, :]) & later[None]
    return jnp.where(allowed[:, None, None], scores, NEG)


def head_norm_back(grad_rot, raw, rinv, gain, cosine, sine):
    grad_normed = rotate_back(grad_rot, cosine, sine)
    gain_grad = jnp.sum(grad_normed * raw * rinv, axis=(0, 1, 2))
    scaled = grad_normed * gain
    grad_raw = rinv * scaled - raw * rinv**3 * jnp.mean(scaled * raw, axis=-1, keepdims=True)
    return (grad_raw, gain_grad)


def row_norm_back(grad_normed, raw, rinv, gain):
    gain_grad = jnp.sum(grad_normed * raw * rinv, axis=0)
    scaled = grad_normed * gain
    grad_raw = rinv * scaled - raw * rinv**3 * jnp.mean(scaled * raw, axis=-1, keepdims=True)
    return (grad_raw, gain_grad)


def left_product(left, right):
    return lax.dot_general(
        left, right, (((0,), (0,)), ((), ())), preferred_element_type=jnp.float32
    )


def right_product(left, right):
    return lax.dot_general(
        left, right, (((1,), (1,)), ((), ())), preferred_element_type=jnp.float32
    )


ALL = ("fsdp", "expert")
WIDE = 512


def after(value, *earlier):
    return lax.optimization_barrier((value, *earlier))[0]


def gather_kernel(place_ref, block_ref, *out_refs):
    block = block_ref[...]
    for d, out_ref in enumerate(out_refs):
        out_ref[...] = jnp.dot(place_ref[0, d], block, preferred_element_type=jnp.float32).astype(jnp.bfloat16)


def gather_slots(place, k, block):
    _, near, cap, count = place.shape
    width = block.shape[1]
    return pl.pallas_call(
        gather_kernel,
        grid=(width // WIDE,),
        in_specs=[
            pl.BlockSpec((1, near, cap, count), lambda j: (k, 0, 0, 0)),
            pl.BlockSpec((count, WIDE), lambda j: (0, j)),
        ],
        out_specs=[pl.BlockSpec((cap, WIDE), lambda j: (0, j))] * near,
        out_shape=[jax.ShapeDtypeStruct((cap, width), jnp.bfloat16)] * near,
        cost_estimate=pl.CostEstimate(
            flops=2 * near * cap * count * width,
            bytes_accessed=2 * width * (count + near * cap) + 2 * near * cap * count,
            transcendentals=0,
        ),
        name="gather_slots",
    )(place, block)


def combine_kernel(weighted, *refs):
    spot_ref, out_ref = refs[0], refs[-1]
    total = None
    for d, piece_ref in enumerate(refs[1 + weighted : -1]):
        piece = piece_ref[...]
        terms = [spot_ref[0, d]]
        if weighted:
            weight = terms[0].astype(jnp.float32) * refs[1][0][:, d : d + 1]
            high = weight.astype(jnp.bfloat16)
            terms = [high, (weight - high.astype(jnp.float32)).astype(jnp.bfloat16)]
        for term in terms:
            part = jnp.dot(term, piece, preferred_element_type=jnp.float32)
            total = part if total is None else total + part
    out_ref[...] = total.astype(out_ref.dtype)


def combine_slots(spot, k, pieces, dtype, gates=None):
    _, near, count, cap = spot.shape
    width = pieces[0].shape[1]
    weighted = gates is not None
    extra = [gates] if weighted else []
    return pl.pallas_call(
        lambda *refs: combine_kernel(int(weighted), *refs),
        grid=(width // WIDE,),
        in_specs=[pl.BlockSpec((1, near, count, cap), lambda j: (k, 0, 0, 0))]
        + [pl.BlockSpec((1, count, near), lambda j: (k, 0, 0))] * weighted
        + [pl.BlockSpec((cap, WIDE), lambda j: (0, j))] * near,
        out_specs=pl.BlockSpec((count, WIDE), lambda j: (0, j)),
        out_shape=jax.ShapeDtypeStruct((count, width), dtype),
        cost_estimate=pl.CostEstimate(
            flops=2 * near * cap * count * width * (1 + weighted),
            bytes_accessed=2 * width * (count + near * cap) + 2 * near * cap * count,
            transcendentals=0,
        ),
        name="combine_slots",
    )(spot, *extra, *pieces)


def on_device(
    tokens,
    segments,
    routes,
    attn_gain,
    w_query,
    key_matrix,
    value_matrix,
    output_matrix,
    query_gain,
    key_gain,
    ffn_gain,
    w_router,
    w_gate,
    w_up,
    w_down,
    cotangent,
):
    nf, ne = lax.axis_size("fsdp"), lax.axis_size("expert")
    nz = ne // 2
    f, e = lax.axis_index("fsdp"), lax.axis_index("expert")
    z, c = e // 2, e % 2
    count = tokens.shape[0]
    experts = nf * ne
    cap = 5 * count * TOP // (4 * experts)
    peers = [(df, dc) for df in range(nf) for dc in range(2)]
    near = len(peers)

    def across(value, df, dc):
        return lax.ppermute(
            value, ALL, [(i * ne + j, (i ^ df) * ne + (j ^ dc)) for i in range(nf) for j in range(ne)]
        )

    def along(value, k):
        return lax.ppermute(value, "expert", [(j, (j + 2 * k) % ne) for j in range(ne)])

    def group_blocks(value):
        return [value] + [across(value, df, 0) for df in range(1, nf)]

    def plane_blocks(value):
        return [value] + [along(value, k) for k in range(1, nz)]

    def place_block(whole, block, plane, core):
        return lax.dynamic_update_slice(whole, block[None, None], (plane, core, 0, 0))

    def gather_rows(value, blocks):
        whole = jnp.zeros((nz, 2) + value.shape, value.dtype)
        for k, block in enumerate(blocks):
            plane = (z - k) % nz
            whole = place_block(whole, block, plane, c)
            whole = place_block(whole, across(block, 0, 1), plane, 1 - c)
        return whole.reshape(ne * value.shape[0], value.shape[1])

    def reduce_rows(grad):
        grad = grad.reshape(nz, 2, grad.shape[0] // ne, grad.shape[1])
        theirs = lax.dynamic_index_in_dim(grad, 1 - c, 1, keepdims=False).astype(jnp.bfloat16)
        mine = lax.dynamic_index_in_dim(grad, c, 1, keepdims=False)
        mine = mine + across(theirs, 0, 1).astype(jnp.float32)
        total = lax.dynamic_index_in_dim(mine, z, 0, keepdims=False)
        for k in range(1, nz):
            part = lax.dynamic_index_in_dim(mine, (z + k) % nz, 0, keepdims=False)
            total = total + along(part.astype(jnp.bfloat16), k).astype(jnp.float32)
        return total

    def sum_blocks(wide):
        rows = wide.shape[0] // nf
        total = wide[:rows].astype(jnp.float32)
        for df in range(1, nf):
            part = wide[df * rows : (df + 1) * rows].astype(jnp.bfloat16)
            total = total + across(part, df, 0).astype(jnp.float32)
        return total

    def sum_all(value):
        for axis, size in (("expert", ne), ("fsdp", nf)):
            step = 1
            while step < size:
                value = value + lax.ppermute(value, axis, [(j, j ^ step) for j in range(size)])
                step *= 2
        return value

    width_q, width_k = w_query.shape[1], key_matrix.shape[1]
    w_heads = jnp.concatenate([w_query, key_matrix, value_matrix], axis=1)
    token_blocks = group_blocks(tokens)
    segment_blocks = group_blocks(segments)
    heads_blocks = plane_blocks(w_heads)
    route_blocks = plane_blocks(jnp.transpose(routes))
    head_blocks = plane_blocks(after(output_matrix, *heads_blocks[1:]))
    cot_blocks = plane_blocks(after(cotangent, *head_blocks[1:]))
    gain_one = lax.all_gather(attn_gain, "expert", axis=0, tiled=True).astype(jnp.float32)
    gain_two = lax.all_gather(ffn_gain, "expert", axis=0, tiled=True).astype(jnp.float32)
    full_router = lax.all_gather(w_router, "expert", axis=0, tiled=True)

    peer_experts = jnp.stack([(f ^ df) * ne + 2 * z + (c ^ dc) for df, dc in peers])
    named = jnp.stack(route_blocks)
    hit = jnp.any(named[:, None] == peer_experts[None, :, None, None], axis=2)
    upto = (jnp.arange(count)[:, None] <= jnp.arange(count)[None, :]).astype(jnp.bfloat16)
    rank = jnp.dot(
        hit.astype(jnp.bfloat16).reshape(nz * near, count), upto, preferred_element_type=jnp.float32
    ).reshape(nz, near, count)
    slot_of = jnp.where(hit, rank - 1.0, -1.0)
    slots = jnp.arange(cap, dtype=jnp.float32)
    place = (slot_of[:, :, None, :] == slots[None, None, :, None]).astype(jnp.bfloat16)
    spot = (slot_of[:, :, :, None] == slots[None, None, None, :]).astype(jnp.bfloat16)

    def send_out(pieces):
        return [across(piece, df, dc) if df or dc else piece for piece, (df, dc) in zip(pieces, peers)]

    scale = HEAD_SIZE ** (-0.5)
    local_q = width_q // HEAD_SIZE
    local_kv = width_k // HEAD_SIZE
    query_groups = local_q // local_kv
    w_heads = gather_rows(w_heads, heads_blocks)
    wide_group = jnp.concatenate(token_blocks, axis=0).astype(jnp.float32)
    group_rinv = inverse_norm(wide_group)
    wide_in, rinv_one = wide_group[:count], group_rinv[:count]
    group_in = (wide_group * group_rinv * gain_one).astype(jnp.bfloat16)
    group_seg = jnp.concatenate(segment_blocks, axis=0)
    rows_all = group_in.shape[0]
    batch_size = rows_all // SEQ
    heads = jnp.dot(group_in, w_heads, preferred_element_type=jnp.float32)
    query = heads[:, :width_q].reshape(batch_size, SEQ, local_q, HEAD_SIZE)
    key_rows = heads[:, width_q : width_q + width_k].reshape(batch_size, SEQ, local_kv, HEAD_SIZE)
    value_rows = heads[:, width_q + width_k :].astype(jnp.bfloat16).reshape(batch_size, SEQ, local_kv, HEAD_SIZE)
    q_rinv = inverse_norm(query)
    k_rinv = inverse_norm(key_rows)
    cosine, sine = rotary_tables(SEQ, HEAD_SIZE)
    q_scale = query_gain.astype(jnp.float32)
    k_scale = key_gain.astype(jnp.float32)
    query_rotated = rotate(query * q_rinv * q_scale, cosine, sine).astype(jnp.bfloat16)
    k_rot = rotate(key_rows * k_rinv * k_scale, cosine, sine).astype(jnp.bfloat16)
    masked = masked_scores(query_rotated, k_rot, group_seg)
    top = jnp.max(masked, axis=-1, keepdims=True)
    lse = top + jnp.log(jnp.sum(jnp.exp(masked - top), axis=-1, keepdims=True))
    prob_low = jnp.exp(masked - lse).astype(jnp.bfloat16)
    mixed = jnp.einsum(
        "bkgqs,bskd->bqkgd", prob_low, value_rows, preferred_element_type=jnp.float32
    ).astype(jnp.bfloat16)
    mixed_flat = mixed.reshape(rows_all, local_q * HEAD_SIZE)
    head_out = gather_rows(output_matrix, head_blocks)
    partial_mid = jnp.dot(mixed_flat, head_out, preferred_element_type=jnp.float32)
    residual_mid = wide_in + sum_blocks(partial_mid)

    rinv_two = inverse_norm(residual_mid)
    normed_two = (residual_mid * rinv_two * gain_two).astype(jnp.bfloat16)
    normed_blocks = plane_blocks(normed_two)
    early = gather_slots(place, 0, after(cotangent, *token_blocks[1:]))
    cot_pieces = [send_out(early)]
    arrived_pieces = []
    last = partial_mid
    for k in range(nz):
        if k:
            pieces = gather_slots(place, k, after(cot_blocks[k], last))
            cot_pieces.append(send_out(pieces))
        pieces = gather_slots(place, k, after(normed_blocks[k], cot_pieces[-1][0]) if k > 1 else normed_blocks[k])
        last = pieces[0]
        arrived_pieces.append(send_out(pieces))

    def gates_of(rows, named_rows):
        logits = jnp.dot(rows, full_router, preferred_element_type=jnp.float32)
        picked = jnp.any(named_rows[:, :, None] == jnp.arange(experts)[None, None, :], axis=0)
        highest = jnp.max(jnp.where(picked, logits, NEG), axis=-1, keepdims=True)
        raised = jnp.where(picked, jnp.exp(jnp.minimum(logits - highest, 0.0)), 0.0)
        return raised / jnp.sum(raised, axis=-1, keepdims=True)

    is_peer = peer_experts[None, :, None] == jnp.arange(experts)[None, None, :]
    peer_gates, gate_columns = [], []
    for k in range(nz):
        all_gates = gates_of(normed_blocks[k], route_blocks[k])
        if k == 0:
            gates = all_gates
        mine = jnp.sum(jnp.where(is_peer, all_gates[:, None, :], 0.0), axis=-1)
        peer_gates.append(mine)
        slot_gates = jnp.sum(place[k].astype(jnp.float32) * jnp.transpose(mine)[:, None, :], axis=-1)
        gate_columns.append(slot_gates)
    gate_columns = jnp.stack(gate_columns, axis=1)
    gate_columns = jnp.stack(send_out([gate_columns[d] for d in range(near)]), axis=1)
    peer_gates = jnp.stack(peer_gates)

    gate_w = w_gate[0]
    up_w = w_up[0]
    down_w = w_down[0]
    saved = []
    out_pieces, slot_d_gates, parts = [], [], []
    for k in range(nz):
        arrived = jnp.concatenate(arrived_pieces[k], axis=0)
        wide_cot = jnp.concatenate(cot_pieces[k], axis=0).astype(jnp.float32)
        gate_pre = jnp.dot(arrived, gate_w, preferred_element_type=jnp.float32)
        up_pre = jnp.dot(arrived, up_w, preferred_element_type=jnp.float32)
        sigma = jax.nn.sigmoid(gate_pre)
        act = (gate_pre * sigma * up_pre).astype(jnp.bfloat16)
        expert_out = jnp.dot(act, down_w, preferred_element_type=jnp.float32).astype(jnp.bfloat16)
        slot_d_gates.append(jnp.sum(wide_cot * expert_out.astype(jnp.float32), axis=-1))
        d_expert = (gate_columns[k].reshape(-1)[:, None] * wide_cot).astype(jnp.bfloat16)
        d_act = right_product(d_expert, down_w)
        d_gate_pre = (d_act * up_pre * sigma * (1.0 + gate_pre * (1.0 - sigma))).astype(jnp.bfloat16)
        d_up_pre = (d_act * gate_pre * sigma).astype(jnp.bfloat16)
        d_rows = (right_product(d_gate_pre, gate_w) + right_product(d_up_pre, up_w)).astype(jnp.bfloat16)
        saved.append((arrived, act, d_expert, d_gate_pre, d_up_pre))
        out_pieces.append(expert_out)
        back = send_out([d_rows[d * cap : (d + 1) * cap] for d in range(near)])
        part = combine_slots(spot, k, back, jnp.bfloat16 if k else jnp.float32)
        parts.append(along(part, nz - k).astype(jnp.float32) if k else part)
    d_normed_two = sum(parts[1:], parts[0])

    slot_d_gates = jnp.stack(slot_d_gates).reshape(nz, near, cap)
    slot_d_gates = jnp.stack(send_out([slot_d_gates[:, d] for d in range(near)]), axis=1)
    token_d_gates = jnp.sum(place.astype(jnp.float32) * slot_d_gates[..., None], axis=2)
    d_gates = jnp.zeros((count, experts), jnp.float32)
    for k in range(nz):
        mine = along(token_d_gates[k], nz - k) if k else token_d_gates[0]
        owners = peer_experts + 2 * ((z + k) % nz - z)
        d_gates = d_gates + jnp.sum(
            jnp.where(owners[:, None, None] == jnp.arange(experts)[None, None, :], mine[:, :, None], 0.0), axis=0
        )
    d_logits = (gates * (d_gates - jnp.sum(gates * d_gates, axis=-1, keepdims=True))).astype(jnp.bfloat16)

    arrived, act, d_expert, d_gate_pre, d_up_pre = [
        jnp.concatenate([after(kept[i], saved[-1][-1]) for kept in saved], axis=0) for i in range(5)
    ]
    down_grad = left_product(act, d_expert)
    gate_grad = left_product(arrived, d_gate_pre)
    up_grad = left_product(arrived, d_up_pre)

    router_grad = left_product(normed_two, d_logits)
    d_normed_two = d_normed_two + right_product(d_logits, full_router)
    d_norm_part, gain_two_grad = row_norm_back(d_normed_two, residual_mid, rinv_two, gain_two)
    d_mid = cotangent.astype(jnp.float32) + d_norm_part
    middle_blocks = group_blocks(d_mid.astype(jnp.bfloat16))
    group_dmid = jnp.concatenate(middle_blocks, axis=0)

    moe = None
    for k in range(nz):
        rows = after(out_pieces[k], group_dmid)
        back = send_out([rows[d * cap : (d + 1) * cap] for d in range(near)])
        part = combine_slots(spot, k, back, jnp.bfloat16 if k else jnp.float32, peer_gates)
        part = along(part, nz - k).astype(jnp.float32) if k else part
        moe = part if moe is None else moe + part
    output = (residual_mid + moe).astype(jnp.bfloat16)

    share_out = reduce_rows(left_product(mixed_flat, group_dmid))
    mixed_rows_grad = (
        right_product(group_dmid, head_out)
        .astype(jnp.bfloat16)
        .reshape(batch_size, SEQ, local_kv, query_groups, HEAD_SIZE)
    )
    prob = jnp.exp(masked_scores(query_rotated, k_rot, group_seg) - lse)
    prob_again = prob.astype(jnp.bfloat16)
    value_rows_grad = jnp.einsum(
        "bkgqs,bqkgd->bskd", prob_again, mixed_rows_grad, preferred_element_type=jnp.float32
    )
    d_prob = jnp.einsum(
        "bqkgd,bskd->bkgqs", mixed_rows_grad, value_rows, preferred_element_type=jnp.float32
    )
    delta = jnp.sum(mixed_rows_grad.astype(jnp.float32) * mixed.astype(jnp.float32), axis=-1)
    delta = jnp.transpose(delta, (0, 2, 3, 1))[..., None]
    d_scores = (prob * (d_prob - delta)).astype(jnp.bfloat16)
    grouped_rows = query_rotated.reshape(batch_size, SEQ, local_kv, query_groups, HEAD_SIZE)
    d_qrot = (
        jnp.einsum(
            "bkgqs,bskd->bqkgd", d_scores, k_rot, preferred_element_type=jnp.float32
        ).reshape(batch_size, SEQ, local_q, HEAD_SIZE)
        * scale
    )
    d_krot = (
        jnp.einsum("bkgqs,bqkgd->bskd", d_scores, grouped_rows, preferred_element_type=jnp.float32)
        * scale
    )
    d_query, q_gain_grad = head_norm_back(d_qrot, query, q_rinv, q_scale, cosine, sine)
    key_rows_grad, k_gain_grad = head_norm_back(d_krot, key_rows, k_rinv, k_scale, cosine, sine)
    d_heads = jnp.concatenate(
        [
            d_query.astype(jnp.bfloat16).reshape(rows_all, width_q),
            key_rows_grad.astype(jnp.bfloat16).reshape(rows_all, width_k),
            value_rows_grad.astype(jnp.bfloat16).reshape(rows_all, width_k),
        ],
        axis=1,
    )
    share_heads = reduce_rows(left_product(group_in, d_heads))
    partial_normed = right_product(d_heads, w_heads)
    gain_one_grad = jnp.sum(partial_normed * wide_group * group_rinv, axis=0)
    d_normed_one = sum_blocks(partial_normed)
    d_tokens, _ = row_norm_back(d_normed_one, wide_in, rinv_one, gain_one)
    token_grad = d_mid + d_tokens

    rows_own = MODEL_WIDTH // ne

    def own_rows(value):
        return lax.dynamic_slice_in_dim(value, e * rows_own, rows_own, value.ndim - 1)

    router_sum = sum_all(jnp.concatenate([jnp.transpose(router_grad), gain_two_grad[None]], axis=0))
    gain_sum = sum_all(jnp.concatenate([gain_one_grad, q_gain_grad, k_gain_grad])[None])[0]
    return (
        output,
        token_grad,
        own_rows(gain_sum[:MODEL_WIDTH]),
        share_heads[:, :width_q],
        share_heads[:, width_q : width_q + width_k],
        share_heads[:, width_q + width_k :],
        share_out,
        gain_sum[MODEL_WIDTH : MODEL_WIDTH + HEAD_SIZE],
        gain_sum[MODEL_WIDTH + HEAD_SIZE :],
        own_rows(router_sum[experts]),
        jnp.transpose(own_rows(router_sum[:experts])),
        gate_grad[None],
        up_grad[None],
        down_grad[None],
    )


def solution(mesh):
    return jax.shard_map(
        on_device,
        mesh=mesh,
        in_specs=(
            P(("fsdp", "expert"), None),
            P(("fsdp", "expert"), None),
            P(("fsdp", "expert"), None),
            P("expert"),
            P("expert", "fsdp"),
            P("expert", "fsdp"),
            P("expert", "fsdp"),
            P(("fsdp", "expert"), None),
            P(),
            P(),
            P("expert"),
            P("expert", None),
            P(("fsdp", "expert"), None, None),
            P(("fsdp", "expert"), None, None),
            P(("fsdp", "expert"), None, None),
            P(("fsdp", "expert"), None),
        ),
        out_specs=(
            P(("fsdp", "expert"), None),
            P(("fsdp", "expert"), None),
            P("expert"),
            P("expert", "fsdp"),
            P("expert", "fsdp"),
            P("expert", "fsdp"),
            P(("fsdp", "expert"), None),
            P(),
            P(),
            P("expert"),
            P("expert", None),
            P(("fsdp", "expert"), None, None),
            P(("fsdp", "expert"), None, None),
            P(("fsdp", "expert"), None, None),
        ),
        check_vma=False,
    )
```

```python
import jax
import jax.numpy as jnp
from jax import lax
from jax.experimental import pallas as pl
from jax.experimental.pallas import tpu as pltpu
from jax.sharding import PartitionSpec as P

MODEL_WIDTH = 2048
HEAD_SIZE = 128
TOP = 8
SEQ = 256


EPS = 1e-06
THETA = 1000000.0
NEG = -1e30


def inverse_norm(value):
    return lax.rsqrt(jnp.mean(value * value, axis=-1, keepdims=True) + EPS)


def rotary_tables(sequence_length, width):
    half = width // 2
    inverse = THETA ** (-(jnp.arange(half).astype(jnp.float32) * 2.0 / width))
    angle = jnp.arange(sequence_length).astype(jnp.float32)[:, None] * inverse[None, :]
    return (jnp.cos(angle)[None, :, None, :], jnp.sin(angle)[None, :, None, :])


def row_norm_back(grad_normed, raw, rinv, gain):
    gain_grad = jnp.sum(grad_normed * raw * rinv, axis=0)
    scaled = grad_normed * gain
    grad_raw = rinv * scaled - raw * rinv**3 * jnp.mean(scaled * raw, axis=-1, keepdims=True)
    return (grad_raw, gain_grad)


def left_product(left, right):
    return lax.dot_general(
        left, right, (((0,), (0,)), ((), ())), preferred_element_type=jnp.float32
    )


def right_product(left, right):
    return lax.dot_general(
        left, right, (((1,), (1,)), ((), ())), preferred_element_type=jnp.float32
    )


ALL = ("fsdp", "expert")
WIDE = 512


def after(value, *earlier):
    return lax.optimization_barrier((value, *earlier))[0]


MESH = pl.DeviceIdType.MESH
MOST_VMEM = 62 * 1024 * 1024


def gather_kernel(ks, near, cap, place_ref, *refs):
    block_refs, out_refs = refs[: len(ks)], refs[len(ks) :]
    for i, (k, block_ref) in enumerate(zip(ks, block_refs)):
        for d in range(near):
            out_refs[d][i * cap : (i + 1) * cap, :] = jnp.dot(
                place_ref[k, d], block_ref[...], preferred_element_type=jnp.float32
            ).astype(jnp.bfloat16)


def gather_slots(place, ks, blocks):
    _, near, cap, count = place.shape
    width = blocks[0].shape[1]
    shape = jax.ShapeDtypeStruct((len(ks) * cap, width), jnp.bfloat16)
    return pl.pallas_call(
        lambda *refs: gather_kernel(ks, near, cap, *refs),
        in_specs=[whole_spec(place)] + [whole_spec(block) for block in blocks],
        out_specs=[whole_spec(shape)] * near,
        out_shape=[shape] * near,
        compiler_params=pltpu.CompilerParams(vmem_limit_bytes=MOST_VMEM),
        cost_estimate=pl.CostEstimate(
            flops=2 * len(ks) * near * cap * count * width,
            bytes_accessed=2 * len(ks) * width * (count + near * cap),
            transcendentals=0,
        ),
        name="gather_slots",
    )(place, *blocks)


def combine_kernel(spot_ref, gates_ref, *refs):
    piece_refs, out_ref = refs[:-1], refs[-1]
    total = None
    for d, piece_ref in enumerate(piece_refs):
        weight = spot_ref[0, d].astype(jnp.float32) * gates_ref[0][:, d : d + 1]
        high = weight.astype(jnp.bfloat16)
        for term in (high, (weight - high.astype(jnp.float32)).astype(jnp.bfloat16)):
            part = jnp.dot(term, piece_ref[...], preferred_element_type=jnp.float32)
            total = part if total is None else total + part
    out_ref[...] = total.astype(out_ref.dtype)


def combine_slots(spot, k, pieces, dtype, gates):
    _, near, count, cap = spot.shape
    width = pieces[0].shape[1]
    return pl.pallas_call(
        combine_kernel,
        grid=(width // WIDE,),
        in_specs=[
            pl.BlockSpec((1, near, count, cap), lambda j: (k, 0, 0, 0)),
            pl.BlockSpec((1, count, near), lambda j: (k, 0, 0)),
        ]
        + [pl.BlockSpec((cap, WIDE), lambda j: (k, j))] * near,
        out_specs=pl.BlockSpec((count, WIDE), lambda j: (0, j)),
        out_shape=jax.ShapeDtypeStruct((count, width), dtype),
        cost_estimate=pl.CostEstimate(
            flops=4 * near * cap * count * width,
            bytes_accessed=2 * width * (count + near * cap) + 2 * near * cap * count,
            transcendentals=0,
        ),
        name="combine_slots",
    )(spot, gates, *pieces)


class Place:
    def __init__(self, nf, nz):
        self.f, e = lax.axis_index("fsdp"), lax.axis_index("expert")
        self.z, self.c = e // 2, e % 2
        self.nf, self.nz = nf, nz

    def plane(self, k):
        return {"fsdp": self.f, "expert": lax.rem(self.z + k, self.nz) * 2 + self.c}

    def peer(self, d):
        df, dc = d // 2, d % 2
        core = 1 - self.c if dc else self.c
        return {"fsdp": self.flip(df), "expert": self.z * 2 + core}

    def flip(self, df):
        other, bit = 0, 1
        while bit < self.nf:
            digit = lax.rem(self.f // bit, 2)
            other = other + bit * (1 - digit if df & bit else digit)
            bit *= 2
        return other

    def greet(self):
        barrier = pltpu.get_barrier_semaphore()
        others = [self.plane(k) for k in range(1, self.nz)] + [self.peer(d) for d in range(1, 2 * self.nf)]
        for other in others:
            pl.semaphore_signal(barrier, inc=1, device_id=other, device_id_type=MESH)
        pl.semaphore_wait(barrier, len(others))


def remote(source, target, send, recv, device):
    return pltpu.make_async_remote_copy(
        src_ref=source, dst_ref=target, send_sem=send, recv_sem=recv, device_id=device, device_id_type=MESH
    )


def send_kernel(nf, nz, block_ref, place_ref, arrived_ref, blocks_ref, held, out, z_send, z_recv, sent, got, keep):
    me = Place(nf, nz)
    near = 2 * nf
    me.greet()
    moves = {
        k: remote(block_ref, held.at[k], z_send.at[k], z_recv.at[k], me.plane(k)) for k in range(1, nz)
    }
    for k in range(1, nz):
        moves[k].start()
    own = pltpu.make_async_copy(block_ref, held.at[0], z_recv.at[0])
    own.start()
    for k in range(nz):
        if k:
            moves[k].wait_recv()
        else:
            own.wait()
        pltpu.make_async_copy(held.at[k], blocks_ref.at[k], keep.at[k]).start()
        for d in range(near):
            out[k, d] = jnp.dot(place_ref[k, d], held[k], preferred_element_type=jnp.float32).astype(jnp.bfloat16)
        for d in range(1, near):
            remote(out.at[k, d], arrived_ref.at[k, d], sent.at[k, d], got.at[k, d], me.peer(d)).start()
        pltpu.make_async_copy(out.at[k, 0], arrived_ref.at[k, 0], got.at[k, 0]).start()
    for k in range(nz):
        pltpu.make_async_copy(held.at[k], blocks_ref.at[k], keep.at[k]).wait()
        pltpu.make_async_copy(out.at[k, 0], arrived_ref.at[k, 0], got.at[k, 0]).wait()
        for d in range(1, near):
            remote(out.at[k, d], arrived_ref.at[k, d], sent.at[k, d], got.at[k, d], me.peer(d)).wait()
        if k:
            moves[k].wait_send()


def send_rows(nf, block, place):
    nz, near, cap, count = place.shape
    width = block.shape[1]
    anywhere = pl.BlockSpec(memory_space=pl.ANY)
    return pl.pallas_call(
        lambda *refs: send_kernel(nf, nz, *refs),
        in_specs=[anywhere, whole_spec(place)],
        out_specs=[anywhere, anywhere],
        out_shape=[
            jax.ShapeDtypeStruct((nz, near, cap, width), jnp.bfloat16),
            jax.ShapeDtypeStruct((nz, count, width), jnp.bfloat16),
        ],
        scratch_shapes=[
            pltpu.VMEM((nz, count, width), jnp.bfloat16),
            pltpu.VMEM((nz, near, cap, width), jnp.bfloat16),
            pltpu.SemaphoreType.DMA((nz,)),
            pltpu.SemaphoreType.DMA((nz,)),
            pltpu.SemaphoreType.DMA((nz, near)),
            pltpu.SemaphoreType.DMA((nz, near)),
            pltpu.SemaphoreType.DMA((nz,)),
        ],
        compiler_params=pltpu.CompilerParams(collective_id=0, has_side_effects=True, vmem_limit_bytes=MOST_VMEM),
        cost_estimate=pl.CostEstimate(flops=0, bytes_accessed=400_000_000, transcendentals=0),
        name="send_rows",
    )(block, place)


def return_kernel(nf, nz, rows_ref, spot_ref, own_ref, parts_ref, back, total, part, z_send, z_recv, sent, got):
    me = Place(nf, nz)
    near = 2 * nf
    order = list(range(1, nz)) + [0]
    me.greet()

    def hop(k, d):
        return remote(rows_ref.at[k, d], back.at[k, d], sent.at[k, d], got.at[k, d], me.peer(d))

    def home(k):
        return pltpu.make_async_copy(rows_ref.at[k, 0], back.at[k, 0], got.at[k, 0])

    def along(k):
        return remote(part.at[k - 1], parts_ref.at[k - 1], z_send.at[k - 1], z_recv.at[k - 1], me.plane(nz - k))

    for k in order:
        for d in range(1, near):
            hop(k, d).start()
        home(k).start()
    for k in order:
        home(k).wait()
        for d in range(near):
            if d:
                hop(k, d).wait_recv()
            term = jnp.dot(spot_ref[k, d], back[k, d], preferred_element_type=jnp.float32)
            if d:
                total[...] += term
            else:
                total[...] = term
        if k:
            part[k - 1] = total[...].astype(jnp.bfloat16)
            along(k).start()
        else:
            own_ref[...] = total[...]
    for k in order:
        for d in range(1, near):
            hop(k, d).wait_send()
        if k:
            along(k).wait()


def return_rows(nf, rows, spot):
    nz, near, cap, width = rows.shape
    count = spot.shape[2]
    anywhere = pl.BlockSpec(memory_space=pl.ANY)
    own = jax.ShapeDtypeStruct((count, width), jnp.float32)
    return pl.pallas_call(
        lambda *refs: return_kernel(nf, nz, *refs),
        in_specs=[anywhere, whole_spec(spot)],
        out_specs=[whole_spec(own), anywhere],
        out_shape=[own, jax.ShapeDtypeStruct((nz - 1, count, width), jnp.bfloat16)],
        scratch_shapes=[
            pltpu.VMEM((nz, near, cap, width), jnp.bfloat16),
            pltpu.VMEM((count, width), jnp.float32),
            pltpu.VMEM((nz - 1, count, width), jnp.bfloat16),
            pltpu.SemaphoreType.DMA((nz - 1,)),
            pltpu.SemaphoreType.DMA((nz - 1,)),
            pltpu.SemaphoreType.DMA((nz, near)),
            pltpu.SemaphoreType.DMA((nz, near)),
        ],
        compiler_params=pltpu.CompilerParams(collective_id=1, has_side_effects=True, vmem_limit_bytes=MOST_VMEM),
        cost_estimate=pl.CostEstimate(flops=0, bytes_accessed=400_000_000, transcendentals=0),
        name="return_rows",
    )(rows, spot)


def expert_kernel(k, near, cap, first, me_ref, rows_ref, router_ref, wg_ref, wu_ref, wd_ref, *refs):
    c_refs, refs = refs[:near], refs[near + (0 if first else 6) :]
    back_ref, out_ref, act_ref, de_ref, dgate_ref, dup_ref, out_sum, row_sum = refs
    width = rows_ref.shape[1]
    step = pl.program_id(0)

    @pl.when(step == 0)
    def _():
        for d in range(near):
            at = slice(d * cap, (d + 1) * cap)
            logits = jnp.dot(rows_ref[at, :], router_ref[...], preferred_element_type=jnp.float32)
            picked = c_refs[d][:, width:].astype(jnp.float32) > 0.5
            highest = jnp.max(jnp.where(picked, logits, NEG), axis=-1, keepdims=True)
            raised = jnp.exp(jnp.where(picked, logits - highest, NEG))
            lane = lax.broadcasted_iota(jnp.int32, logits.shape, 1)
            mine = jnp.sum(jnp.where(lane == me_ref[0], raised, 0.0), axis=-1, keepdims=True)
            gate = mine / jnp.maximum(jnp.sum(raised, axis=-1, keepdims=True), 1e-30)
            de_ref[at, :] = (gate * c_refs[d][:, :width].astype(jnp.float32)).astype(jnp.bfloat16)
        out_sum[...] = jnp.zeros_like(out_sum)
        row_sum[...] = jnp.zeros_like(row_sum)

    rows = rows_ref[...]
    wg, wu, wd = wg_ref[0], wu_ref[0], wd_ref[0]
    gate_pre = jnp.dot(rows, wg, preferred_element_type=jnp.float32)
    up_pre = jnp.dot(rows, wu, preferred_element_type=jnp.float32)
    sigma = jax.nn.sigmoid(gate_pre)
    act = (gate_pre * sigma * up_pre).astype(jnp.bfloat16)
    act_ref[...] = act
    out_sum[...] += jnp.dot(act, wd, preferred_element_type=jnp.float32)
    d_act = right_product(de_ref[...], wd)
    d_gate = (d_act * up_pre * sigma * (1.0 + gate_pre * (1.0 - sigma))).astype(jnp.bfloat16)
    d_up = (d_act * gate_pre * sigma).astype(jnp.bfloat16)
    dgate_ref[...] = d_gate
    dup_ref[...] = d_up
    row_sum[...] += right_product(d_gate, wg) + right_product(d_up, wu)

    @pl.when(step == pl.num_programs(0) - 1)
    def _():
        lane = lax.broadcasted_iota(jnp.int32, (cap, back_ref.shape[1] - width), 1)
        for d in range(near):
            at = slice(d * cap, (d + 1) * cap)
            out = out_sum[at, :].astype(jnp.bfloat16)
            out_ref[at, :] = out
            rest = jnp.sum(
                c_refs[d][:, :width].astype(jnp.float32) * out.astype(jnp.float32), axis=-1, keepdims=True
            )
            extra = jnp.zeros(lane.shape, jnp.float32)
            for i in range(3):
                term = rest.astype(jnp.bfloat16).astype(jnp.float32)
                extra = jnp.where(lane == (k * near + d) * 3 + i, term, extra)
                rest = rest - term
            back_ref[at, :width] = row_sum[at, :].astype(jnp.bfloat16)
            back_ref[at, width:] = extra.astype(jnp.bfloat16)


def expert_block(k, nz, me, arrived, router, w_gate, w_up, w_down, cots, at, kept):
    near = len(cots)
    width = arrived.shape[1]
    rows = arrived.shape[0] // nz
    cap = rows // near
    hidden = w_gate.shape[2]
    extra = -(-3 * near * nz // 128) * 128
    tile = 256
    first = kept is None
    before = [] if first else list(kept)
    wide = pl.BlockSpec((rows, width), lambda j: (k, 0))
    narrow = pl.BlockSpec((rows, tile), lambda j: (k, j))
    return pl.pallas_call(
        lambda *refs: expert_kernel(k, near, cap, first, *refs),
        grid=(hidden // tile,),
        in_specs=[
            SCALARS,
            wide,
            pl.BlockSpec(router.shape, lambda j: (0, 0)),
            pl.BlockSpec((1, width, tile), lambda j: (0, 0, j)),
            pl.BlockSpec((1, width, tile), lambda j: (0, 0, j)),
            pl.BlockSpec((1, tile, width), lambda j: (0, j, 0)),
        ]
        + [pl.BlockSpec((cap, cots[0].shape[1]), lambda j: (at, 0), pipeline_mode=pl.Buffered(1))] * near
        + [pl.BlockSpec(memory_space=pl.ANY)] * len(before),
        out_specs=[pl.BlockSpec((rows, width + extra), lambda j: (k, 0)), wide, narrow, wide, narrow, narrow],
        out_shape=[
            jax.ShapeDtypeStruct((nz * rows, n), jnp.bfloat16)
            for n in (width + extra, width, hidden, width, hidden, hidden)
        ],
        scratch_shapes=[pltpu.VMEM((rows, width), jnp.float32)] * 2,
        input_output_aliases={6 + near + i: i for i in range(len(before))},
        compiler_params=pltpu.CompilerParams(vmem_limit_bytes=MOST_VMEM),
        cost_estimate=pl.CostEstimate(
            flops=12 * rows * width * hidden,
            bytes_accessed=6 * width * hidden + 12 * rows * width + 6 * rows * hidden,
            transcendentals=rows * hidden,
        ),
        name="expert_block",
    )(me, arrived, router, w_gate, w_up, w_down, *cots, *before)


def whole_spec(value):
    return pl.BlockSpec(value.shape, lambda *_: (0,) * len(value.shape))


SCALARS = pl.BlockSpec(memory_space=pltpu.SMEM)


def scores_of(q_rot, k_rot, seg_col, seg_row):
    scores = right_product(q_rot, k_rot) * HEAD_SIZE ** (-0.5)
    here = lax.broadcasted_iota(jnp.int32, scores.shape, 0) >= lax.broadcasted_iota(jnp.int32, scores.shape, 1)
    return jnp.where(here & (seg_col == seg_row), scores, NEG)


def turn(value, cos, sin):
    return value * cos + pltpu.roll(value, HEAD_SIZE // 2, 1) * sin


def attend_kernel(blocks, heads, kv_heads, spots, x_ref, gain_ref, row_ref, col_ref, cos_ref, sin_ref, qg_ref, kg_ref, *refs):
    w_refs, refs = refs[:blocks], refs[blocks:]
    normed_ref, raw_ref, rot_ref, value_ref, mixed_ref, lse_ref = refs
    wide = x_ref[...].astype(jnp.float32)
    normed_ref[...] = (wide * inverse_norm(wide) * gain_ref[...]).astype(jnp.bfloat16)
    depth = w_refs[0].shape[0]
    total = None
    for i, w_ref in enumerate(w_refs):
        part = normed_ref[...] if blocks == 1 else normed_ref[:, pl.ds(pl.multiple_of(spots[i] * depth, depth), depth)]
        part = jnp.dot(part, w_ref[...], preferred_element_type=jnp.float32)
        total = part if total is None else total + part
    turned = (heads + kv_heads) * HEAD_SIZE
    raw_ref[...] = total[:, :turned]
    value_ref[...] = total[:, turned:].astype(jnp.bfloat16)
    cos, sin = cos_ref[...], sin_ref[...]
    for h in range(heads + kv_heads):
        at = slice(h * HEAD_SIZE, (h + 1) * HEAD_SIZE)
        raw = raw_ref[:, at]
        gain = qg_ref[...] if h < heads else kg_ref[...]
        rot_ref[:, at] = turn(raw * inverse_norm(raw) * gain, cos, sin).astype(jnp.bfloat16)
    lane = lax.broadcasted_iota(jnp.int32, lse_ref.shape, 1)
    all_lse = jnp.zeros(lse_ref.shape, jnp.float32)
    for h in range(heads):
        at = slice(h * HEAD_SIZE, (h + 1) * HEAD_SIZE)
        g = h * kv_heads // heads
        masked = scores_of(
            rot_ref[:, at],
            rot_ref[:, (heads + g) * HEAD_SIZE : (heads + g + 1) * HEAD_SIZE],
            col_ref[...],
            row_ref[...],
        )
        top = jnp.max(masked, axis=-1, keepdims=True)
        lse = top + jnp.log(jnp.sum(jnp.exp(masked - top), axis=-1, keepdims=True))
        prob_low = jnp.exp(masked - lse).astype(jnp.bfloat16)
        mixed_ref[:, at] = jnp.dot(
            prob_low, value_ref[:, g * HEAD_SIZE : (g + 1) * HEAD_SIZE], preferred_element_type=jnp.float32
        ).astype(jnp.bfloat16)
        all_lse = jnp.where(lane == h, lse, all_lse)
    lse_ref[...] = all_lse


def attend(spots, tokens, gain, seg_row, seg_col, cos, sin, qg, kg, w_blocks, heads, kv_heads):
    count, width = tokens.shape
    args = (tokens, gain, seg_row, seg_col, cos, sin, qg, kg, *w_blocks)
    shapes = [
        jax.ShapeDtypeStruct((count, width), jnp.bfloat16),
        jax.ShapeDtypeStruct((count, (heads + kv_heads) * HEAD_SIZE), jnp.float32),
        jax.ShapeDtypeStruct((count, (heads + kv_heads) * HEAD_SIZE), jnp.bfloat16),
        jax.ShapeDtypeStruct((count, kv_heads * HEAD_SIZE), jnp.bfloat16),
        jax.ShapeDtypeStruct((count, heads * HEAD_SIZE), jnp.bfloat16),
        jax.ShapeDtypeStruct((count, 128), jnp.float32),
    ]
    return pl.pallas_call(
        lambda *refs: attend_kernel(len(w_blocks), heads, kv_heads, *refs),
        in_specs=[SCALARS] + [whole_spec(v) for v in args],
        out_specs=[whole_spec(v) for v in shapes],
        out_shape=shapes,
        cost_estimate=pl.CostEstimate(
            flops=2 * count * width * (heads + 2 * kv_heads) * HEAD_SIZE + 4 * heads * count * count * HEAD_SIZE,
            bytes_accessed=2 * width * (heads + 2 * kv_heads) * HEAD_SIZE + 16 * count * width,
            transcendentals=2 * heads * count * count,
        ),
        name="attend",
    )(spots, *args)


def project_kernel(blocks, spots, mixed_ref, *refs):
    w_refs, out_ref = refs[:blocks], refs[-1]
    depth = w_refs[0].shape[0]
    total = None
    for i, w_ref in enumerate(w_refs):
        part = mixed_ref[...] if blocks == 1 else mixed_ref[:, pl.ds(pl.multiple_of(spots[i] * depth, depth), depth)]
        part = jnp.dot(part, w_ref[...], preferred_element_type=jnp.float32)
        total = part if total is None else total + part
    out_ref[...] = total.astype(out_ref.dtype)


def project(spots, mixed, w_blocks, dtype):
    count, depth = mixed.shape
    width = w_blocks[0].shape[1]
    return pl.pallas_call(
        lambda *refs: project_kernel(len(w_blocks), *refs),
        grid=(width // WIDE,),
        in_specs=[SCALARS, pl.BlockSpec((count, depth), lambda j: (0, 0))]
        + [pl.BlockSpec((w.shape[0], WIDE), lambda j: (0, j)) for w in w_blocks],
        out_specs=pl.BlockSpec((count, WIDE), lambda j: (0, j)),
        out_shape=jax.ShapeDtypeStruct((count, width), dtype),
        cost_estimate=pl.CostEstimate(
            flops=2 * count * depth * width, bytes_accessed=2 * depth * width + 4 * count * width, transcendentals=0
        ),
        name="project",
    )(spots, mixed, *w_blocks)


def head_back(grad_rot, raw, gain, cos, sin):
    grad_normed = turn(grad_rot, cos, -sin)
    rinv = inverse_norm(raw)
    gain_grad = jnp.sum(grad_normed * raw * rinv, axis=0, keepdims=True)
    scaled = grad_normed * gain
    return rinv * scaled - raw * rinv**3 * jnp.mean(scaled * raw, axis=-1, keepdims=True), gain_grad


def attend_back_kernel(
    blocks, heads, kv_heads, spots, dmid_ref, x_ref, row_ref, col_ref, cos_ref, sin_ref, qg_ref, kg_ref,
    raw_ref, rot_ref, value_ref, mixed_ref, lse_ref, *refs
):
    o_refs, w_refs, refs = refs[:blocks], refs[blocks : 2 * blocks], refs[2 * blocks :]
    dheads_ref, part_ref, gain_ref, qgain_ref, kgain_ref, dmixed = refs
    scale = HEAD_SIZE ** (-0.5)
    dmid = dmid_ref[...]
    depth = o_refs[0].shape[0]
    for i, o_ref in enumerate(o_refs):
        part = right_product(dmid, o_ref[...]).astype(jnp.bfloat16)
        if blocks == 1:
            dmixed[...] = part
        else:
            dmixed[:, pl.ds(pl.multiple_of(spots[i] * depth, depth), depth)] = part
    cos, sin = cos_ref[...], sin_ref[...]
    lane = lax.broadcasted_iota(jnp.int32, lse_ref.shape, 1)
    all_lse = lse_ref[...]
    q_gain = jnp.zeros(qgain_ref.shape, jnp.float32)
    k_gain = jnp.zeros(kgain_ref.shape, jnp.float32)
    for g in range(kv_heads):
        kv = slice(g * HEAD_SIZE, (g + 1) * HEAD_SIZE)
        key_at = slice((heads + g) * HEAD_SIZE, (heads + g + 1) * HEAD_SIZE)
        k_rot, value = rot_ref[:, key_at], value_ref[:, kv]
        d_value, d_key = None, None
        for h in range(g * heads // kv_heads, (g + 1) * heads // kv_heads):
            at = slice(h * HEAD_SIZE, (h + 1) * HEAD_SIZE)
            q_rot, grad = rot_ref[:, at], dmixed[:, at]
            lse = jnp.sum(jnp.where(lane == h, all_lse, 0.0), axis=-1, keepdims=True)
            prob = jnp.exp(scores_of(q_rot, k_rot, col_ref[...], row_ref[...]) - lse)
            part = left_product(prob.astype(jnp.bfloat16), grad)
            d_value = part if d_value is None else d_value + part
            d_prob = right_product(grad, value)
            delta = jnp.sum(grad.astype(jnp.float32) * mixed_ref[:, at].astype(jnp.float32), axis=-1, keepdims=True)
            d_scores = (prob * (d_prob - delta)).astype(jnp.bfloat16)
            part = left_product(d_scores, q_rot)
            d_key = part if d_key is None else d_key + part
            d_q = jnp.dot(d_scores, k_rot, preferred_element_type=jnp.float32) * scale
            d_query, gain_part = head_back(d_q, raw_ref[:, at], qg_ref[...], cos, sin)
            q_gain = q_gain + gain_part
            dheads_ref[:, at] = d_query.astype(jnp.bfloat16)
        d_key, gain_part = head_back(d_key * scale, raw_ref[:, key_at], kg_ref[...], cos, sin)
        k_gain = k_gain + gain_part
        dheads_ref[:, key_at] = d_key.astype(jnp.bfloat16)
        last = (heads + kv_heads + g) * HEAD_SIZE
        dheads_ref[:, last : last + HEAD_SIZE] = d_value.astype(jnp.bfloat16)
    qgain_ref[...] = q_gain
    kgain_ref[...] = k_gain
    d_heads = dheads_ref[...]
    wide = x_ref[...].astype(jnp.float32)
    rinv = inverse_norm(wide)
    depth = w_refs[0].shape[0]
    for i, w_ref in enumerate(w_refs):
        part = right_product(d_heads, w_ref[...])
        at = slice(None) if blocks == 1 else pl.ds(pl.multiple_of(spots[i] * depth, depth), depth)
        part_ref[:, at] = part.astype(part_ref.dtype)
        x = x_ref[:, at].astype(jnp.float32)
        gain_ref[:, at] = jnp.sum(part * x * rinv, axis=0, keepdims=True)


def attend_back(spots, dmid, tokens, seg_row, seg_col, cos, sin, qg, kg, saved, o_blocks, w_blocks, heads, kv_heads, dtype):
    count, width = tokens.shape
    args = (dmid, tokens, seg_row, seg_col, cos, sin, qg, kg, *saved, *o_blocks, *w_blocks)
    lanes = (heads + 2 * kv_heads) * HEAD_SIZE
    shapes = [
        jax.ShapeDtypeStruct((count, lanes), jnp.bfloat16),
        jax.ShapeDtypeStruct((count, width), dtype),
        jax.ShapeDtypeStruct((1, width), jnp.float32),
        jax.ShapeDtypeStruct((1, HEAD_SIZE), jnp.float32),
        jax.ShapeDtypeStruct((1, HEAD_SIZE), jnp.float32),
    ]
    return pl.pallas_call(
        lambda *refs: attend_back_kernel(len(w_blocks), heads, kv_heads, *refs),
        in_specs=[SCALARS] + [whole_spec(v) for v in args],
        out_specs=[whole_spec(v) for v in shapes],
        out_shape=shapes,
        scratch_shapes=[pltpu.VMEM((count, heads * HEAD_SIZE), jnp.bfloat16)],
        cost_estimate=pl.CostEstimate(
            flops=4 * count * width * lanes + 10 * heads * count * count * HEAD_SIZE,
            bytes_accessed=4 * width * lanes + 24 * count * width,
            transcendentals=heads * count * count,
        ),
        name="attend_back",
    )(spots, *args)


def on_device(
    tokens,
    segments,
    routes,
    attn_gain,
    w_query,
    key_matrix,
    value_matrix,
    output_matrix,
    query_gain,
    key_gain,
    ffn_gain,
    w_router,
    w_gate,
    w_up,
    w_down,
    cotangent,
):
    nf, ne = lax.axis_size("fsdp"), lax.axis_size("expert")
    nz = ne // 2
    f, e = lax.axis_index("fsdp"), lax.axis_index("expert")
    z, c = e // 2, e % 2
    count = tokens.shape[0]
    experts = nf * ne
    cap = -(5 * count * TOP // (4 * experts)) // 16 * -16
    peers = [(df, dc) for df in range(nf) for dc in range(2)]
    near = len(peers)

    def across(value, df, dc):
        return lax.ppermute(
            value, ALL, [(i * ne + j, (i ^ df) * ne + (j ^ dc)) for i in range(nf) for j in range(ne)]
        )

    def along(value, k):
        return lax.ppermute(value, "expert", [(j, (j + 2 * k) % ne) for j in range(ne)])

    def group_blocks(value):
        return [value] + [across(value, df, 0) for df in range(1, nf)]

    def plane_blocks(value):
        return [value] + [along(value, k) for k in range(1, nz)]

    def spread_rows(blocks):
        rows, width = blocks[0].shape
        places, pieces = [], []
        for k, block in enumerate(blocks):
            places += [(z - k) % nz * 2 + c, (z - k) % nz * 2 + 1 - c]
            pieces += [block, across(block, 0, 1)]
        if rows % 128 == 0:
            return pieces, jnp.stack(places).astype(jnp.int32)
        whole = jnp.zeros((ne, rows, width), blocks[0].dtype)
        for at, piece in zip(places, pieces):
            whole = lax.dynamic_update_slice(whole, piece[None], (at, 0, 0))
        return [whole.reshape(ne * rows, width)], jnp.zeros((1,), jnp.int32)

    def reduce_rows(grad, *earlier):
        grad = grad.reshape(nz, 2, grad.shape[0] // ne, grad.shape[1])
        theirs = lax.dynamic_index_in_dim(grad, 1 - c, 1, keepdims=False).astype(jnp.bfloat16)
        mine = lax.dynamic_index_in_dim(grad, c, 1, keepdims=False)
        mine = mine + across(theirs, 0, 1).astype(jnp.float32)
        total = lax.dynamic_index_in_dim(mine, z, 0, keepdims=False)
        parts = [lax.dynamic_index_in_dim(mine, (z + k) % nz, 0, keepdims=False) for k in range(1, nz)]
        parts = [after(part.astype(jnp.bfloat16), *earlier) for part in parts]
        for k, part in enumerate(parts, 1):
            total = total + along(part, k).astype(jnp.float32)
        return total, parts

    def sum_over(value, axis, size):
        step = 1
        while step < size:
            value = value + lax.ppermute(value, axis, [(j, j ^ step) for j in range(size)])
            step *= 2
        return value

    width_q, width_k = w_query.shape[1], key_matrix.shape[1]
    w_heads = jnp.concatenate([w_query, key_matrix, value_matrix], axis=1)
    token_blocks = group_blocks(tokens)
    segment_blocks = group_blocks(segments)
    few = jnp.concatenate(
        [jnp.transpose(routes).astype(jnp.bfloat16).reshape(-1, w_router.shape[0]), attn_gain[None], ffn_gain[None], jnp.transpose(w_router)]
    )
    few_blocks = plane_blocks(few)
    heads_blocks = plane_blocks(after(w_heads, few))
    few_pairs = across(jnp.stack([block[-experts - 2 :] for block in few_blocks]), 0, 1)
    few_whole = jnp.zeros((nz, 2) + few_pairs.shape[1:], jnp.bfloat16)
    for k, block in enumerate(few_blocks):
        for core, piece in ((c, block[-experts - 2 :]), (1 - c, few_pairs[k])):
            few_whole = lax.dynamic_update_slice(few_whole, piece[None, None], ((z - k) % nz, core, 0, 0))
    few_whole = jnp.transpose(few_whole, (2, 0, 1, 3)).reshape(experts + 2, MODEL_WIDTH)
    gain_one, gain_two = few_whole[:1].astype(jnp.float32), few_whole[1:2].astype(jnp.float32)
    full_router = jnp.transpose(jnp.pad(few_whole[2:], ((0, -experts % 128), (0, 0))))
    route_blocks = [block[: -experts - 2].reshape(TOP, count).astype(jnp.int32) for block in few_blocks]
    head_blocks = plane_blocks(after(output_matrix, *heads_blocks[1:]))
    picked = jnp.any(routes[:, :, None] == jnp.arange(full_router.shape[1])[None, None, :], axis=1)
    cot_wide = jnp.concatenate([cotangent, picked.astype(jnp.bfloat16)], axis=1)
    cot_blocks = plane_blocks(after(cot_wide, *head_blocks[1:]))

    peer_experts = jnp.stack([(f ^ df) * ne + 2 * z + (c ^ dc) for df, dc in peers])
    named = jnp.stack(route_blocks)
    hit = jnp.any(named[:, None] == peer_experts[None, :, None, None], axis=2)
    upto = (jnp.arange(count)[:, None] <= jnp.arange(count)[None, :]).astype(jnp.bfloat16)
    rank = jnp.dot(
        hit.astype(jnp.bfloat16).reshape(nz * near, count), upto, preferred_element_type=jnp.float32
    ).reshape(nz, near, count)
    slot_of = jnp.where(hit, rank - 1.0, -1.0)
    slots = jnp.arange(cap, dtype=jnp.float32)
    place = (slot_of[:, :, None, :] == slots[None, None, :, None]).astype(jnp.bfloat16)
    spot = (slot_of[:, :, :, None] == slots[None, None, None, :]).astype(jnp.bfloat16)

    def send_out(pieces):
        return [across(piece, df, dc) if df or dc else piece for piece, (df, dc) in zip(pieces, peers)]

    local_q = width_q // HEAD_SIZE
    local_kv = width_k // HEAD_SIZE
    w_blocks, spots = spread_rows(heads_blocks)
    cosine, sine = rotary_tables(SEQ, HEAD_SIZE)
    cos = jnp.concatenate([cosine[0, :, 0], cosine[0, :, 0]], axis=-1)
    sin = jnp.concatenate([-sine[0, :, 0], sine[0, :, 0]], axis=-1)
    q_scale = query_gain.astype(jnp.float32)[None]
    k_scale = key_gain.astype(jnp.float32)[None]
    turns = [1 + df for df in range(nf - 1)] + [0]
    shared = [
        (segment_blocks[df], jnp.transpose(segment_blocks[df]), cos, sin, q_scale, k_scale) for df in range(nf)
    ]
    attended = [None] * nf
    for df in turns:
        attended[df] = attend(
            spots, token_blocks[df], gain_one, *shared[df], w_blocks, local_q, local_kv
        )
    o_blocks, _ = spread_rows([after(block, attended[turns[0]][0]) for block in head_blocks])
    wide_in = tokens.astype(jnp.float32)
    rinv_one = inverse_norm(wide_in)
    residual_mid = wide_in
    for df in turns:
        part = project(spots, attended[df][4], o_blocks, jnp.bfloat16 if df else jnp.float32)
        if df:
            part = across(part, df, 0).astype(jnp.float32)
        residual_mid = residual_mid + part
        partial_mid = part

    rinv_two = inverse_norm(residual_mid)
    normed_two = (residual_mid * rinv_two * gain_two).astype(jnp.bfloat16)
    early = gather_slots(place, (0,), [after(cot_wide, *token_blocks[1:])])
    early = send_out(early)
    others = tuple(range(1, nz))
    late = gather_slots(place, others, [after(cot_blocks[k], partial_mid) for k in others])
    late = send_out(late)
    arrived, normed_blocks = send_rows(nf, after(normed_two, late[0]), place)

    me = (f * ne + e).astype(jnp.int32)[None]
    kept = None
    for k in range(nz):
        kept = expert_block(
            k,
            nz,
            me,
            arrived.reshape(nz * near * cap, MODEL_WIDTH),
            full_router,
            w_gate,
            w_up,
            w_down,
            late if k else early,
            max(k - 1, 0),
            kept,
        )
    d_rows, expert_out, act, d_expert, d_gate_pre, d_up_pre = kept
    own_sum, plane_sums = return_rows(nf, d_rows.reshape(nz, near, cap, d_rows.shape[1]), spot)
    back_sum = own_sum + jnp.sum(plane_sums.astype(jnp.float32), axis=0)
    d_normed_two = back_sum[:, :MODEL_WIDTH]

    def gates_of(rows, named_rows):
        logits = jnp.dot(rows, full_router, preferred_element_type=jnp.float32)[:, :experts]
        picked = jnp.any(named_rows[:, :, None] == jnp.arange(experts)[None, None, :], axis=0)
        highest = jnp.max(jnp.where(picked, logits, NEG), axis=-1, keepdims=True)
        raised = jnp.where(picked, jnp.exp(jnp.minimum(logits - highest, 0.0)), 0.0)
        return raised / jnp.sum(raised, axis=-1, keepdims=True)

    gates = gates_of(normed_two, route_blocks[0])

    owners = jnp.concatenate(
        [jnp.repeat(peer_experts + 2 * ((z + k) % nz - z), 3) for k in range(nz)]
    )
    names = (owners[:, None] == jnp.arange(experts)[None, :]).astype(jnp.float32)
    d_gates = jnp.dot(
        back_sum[:, MODEL_WIDTH : MODEL_WIDTH + 3 * near * nz], names, precision=lax.Precision.HIGHEST
    )
    d_logits = (gates * (d_gates - jnp.sum(gates * d_gates, axis=-1, keepdims=True))).astype(jnp.bfloat16)

    router_grad = left_product(normed_two, d_logits)
    d_normed_two = d_normed_two + right_product(d_logits, full_router[:, :experts])
    d_norm_part, gain_two_grad = row_norm_back(d_normed_two, residual_mid, rinv_two, gain_two)
    d_mid = cotangent.astype(jnp.float32) + d_norm_part
    middle_blocks = group_blocks(d_mid.astype(jnp.bfloat16))
    router_sum = after(jnp.concatenate([jnp.transpose(router_grad), gain_two_grad[None]], axis=0), middle_blocks[0])
    router_sum = sum_over(sum_over(router_sum, "expert", ne), "fsdp", nf)
    arrived, act, d_expert, d_gate_pre, d_up_pre = after(
        (arrived.reshape(act.shape[0], MODEL_WIDTH), act, d_expert, d_gate_pre, d_up_pre), middle_blocks[0]
    )
    down_grad = left_product(act, d_expert)
    gate_grad = left_product(arrived, d_gate_pre)
    up_grad = left_product(arrived, d_up_pre)

    is_peer = peer_experts[None, :, None] == jnp.arange(experts)[None, None, :]
    peer_gates = jnp.stack(
        [
            jnp.sum(jnp.where(is_peer, gates_of(normed_blocks[k], route_blocks[k])[:, None, :], 0.0), axis=-1)
            for k in range(nz)
        ]
    )
    expert_out = after(expert_out, router_sum, *middle_blocks[1:]).reshape(nz, near, cap, MODEL_WIDTH)
    back = send_out([expert_out[:, d].reshape(nz * cap, MODEL_WIDTH) for d in range(near)])
    mixed = jnp.concatenate([attended[df][4] for df in range(nf)], axis=0)
    share_out, out_parts = reduce_rows(left_product(mixed, jnp.concatenate(middle_blocks, axis=0)))
    d_heads = [None] * nf
    d_normed_one, gain_one_grad, q_gain_grad, k_gain_grad = None, None, None, None
    for df in range(nf):
        d_heads[df], part, *sums = attend_back(
            spots,
            middle_blocks[df],
            token_blocks[df],
            *shared[df],
            attended[df][1:],
            o_blocks,
            w_blocks,
            local_q,
            local_kv,
            jnp.bfloat16 if df else jnp.float32,
        )
        if df:
            part = across(part, df, 0).astype(jnp.float32)
            d_normed_one = d_normed_one + part
            gain_one_grad, q_gain_grad, k_gain_grad = [
                a + b for a, b in zip((gain_one_grad, q_gain_grad, k_gain_grad), sums)
            ]
        else:
            d_normed_one = part
            gain_one_grad, q_gain_grad, k_gain_grad = sums
    normed_one = jnp.concatenate([attended[df][0] for df in range(nf)], axis=0)
    gain_columns = jnp.concatenate([gain_one_grad, q_gain_grad, k_gain_grad], axis=1)
    gain_columns = sum_over(gain_columns, "expert", ne)
    share_heads, head_parts = reduce_rows(
        left_product(normed_one, jnp.concatenate(d_heads, axis=0)), gain_columns
    )
    peer_gates = after(peer_gates, *out_parts, *head_parts)
    moe = None
    for k in list(range(1, nz)) + [0]:
        part = combine_slots(spot, k, back, jnp.bfloat16 if k else jnp.float32, peer_gates)
        part = along(part, nz - k).astype(jnp.float32) if k else part
        moe = part if moe is None else moe + part
    output = (residual_mid + moe).astype(jnp.bfloat16)

    d_tokens, _ = row_norm_back(d_normed_one, wide_in, rinv_one, gain_one)
    token_grad = d_mid + d_tokens

    rows_own = MODEL_WIDTH // ne

    def own_rows(value):
        return lax.dynamic_slice_in_dim(value, e * rows_own, rows_own, value.ndim - 1)

    gain_sum = sum_over(gain_columns, "fsdp", nf)[0]
    return (
        output,
        token_grad,
        own_rows(gain_sum[:MODEL_WIDTH]),
        share_heads[:, :width_q],
        share_heads[:, width_q : width_q + width_k],
        share_heads[:, width_q + width_k :],
        share_out,
        gain_sum[MODEL_WIDTH : MODEL_WIDTH + HEAD_SIZE],
        gain_sum[MODEL_WIDTH + HEAD_SIZE :],
        own_rows(router_sum[experts]),
        jnp.transpose(own_rows(router_sum[:experts])),
        gate_grad[None],
        up_grad[None],
        down_grad[None],
    )


def solution(mesh):
    return jax.shard_map(
        on_device,
        mesh=mesh,
        in_specs=(
            P(("fsdp", "expert"), None),
            P(("fsdp", "expert"), None),
            P(("fsdp", "expert"), None),
            P("expert"),
            P("expert", "fsdp"),
            P("expert", "fsdp"),
            P("expert", "fsdp"),
            P(("fsdp", "expert"), None),
            P(),
            P(),
            P("expert"),
            P("expert", None),
            P(("fsdp", "expert"), None, None),
            P(("fsdp", "expert"), None, None),
            P(("fsdp", "expert"), None, None),
            P(("fsdp", "expert"), None),
        ),
        out_specs=(
            P(("fsdp", "expert"), None),
            P(("fsdp", "expert"), None),
            P("expert"),
            P("expert", "fsdp"),
            P("expert", "fsdp"),
            P("expert", "fsdp"),
            P(("fsdp", "expert"), None),
            P(),
            P(),
            P("expert"),
            P("expert", None),
            P(("fsdp", "expert"), None, None),
            P(("fsdp", "expert"), None, None),
            P(("fsdp", "expert"), None, None),
        ),
        check_vma=False,
    )
```

```python
import jax
import jax.numpy as jnp
from jax import lax
from jax.experimental import pallas as pl
from jax.experimental.pallas import tpu as pltpu
from jax.sharding import PartitionSpec as P


MODEL_WIDTH = 2048
HEAD_SIZE = 128
TOP = 8
SEQ = 256


EPS = 1e-06
THETA = 1000000.0
NEG = -1e30


def inverse_norm(value):
    return lax.rsqrt(jnp.mean(value * value, axis=-1, keepdims=True) + EPS)


def rotary_tables(sequence_length, width):
    half = width // 2
    inverse = THETA ** (-(jnp.arange(half).astype(jnp.float32) * 2.0 / width))
    angle = jnp.arange(sequence_length).astype(jnp.float32)[:, None] * inverse[None, :]
    return (jnp.cos(angle)[None, :, None, :], jnp.sin(angle)[None, :, None, :])


def row_norm_back(grad_normed, raw, rinv, gain):
    gain_grad = jnp.sum(grad_normed * raw * rinv, axis=0)
    scaled = grad_normed * gain
    grad_raw = rinv * scaled - raw * rinv**3 * jnp.mean(scaled * raw, axis=-1, keepdims=True)
    return (grad_raw, gain_grad)


def left_product(left, right):
    return lax.dot_general(
        left, right, (((0,), (0,)), ((), ())), preferred_element_type=jnp.float32
    )


def right_product(left, right):
    return lax.dot_general(
        left, right, (((1,), (1,)), ((), ())), preferred_element_type=jnp.float32
    )


ALL = ("fsdp", "expert")
WIDE = 512


def after(value, *earlier):
    return lax.optimization_barrier((value, *earlier))[0]


MESH = pl.DeviceIdType.MESH
MOST_VMEM = 62 * 1024 * 1024


def gather_kernel(ks, near, cap, place_ref, *refs):
    block_refs, out_refs = refs[: len(ks)], refs[len(ks) :]
    for i, (k, block_ref) in enumerate(zip(ks, block_refs)):
        for d in range(near):
            out_refs[d][i * cap : (i + 1) * cap, :] = jnp.dot(
                place_ref[k, d], block_ref[...], preferred_element_type=jnp.float32
            ).astype(jnp.bfloat16)


def gather_slots(place, ks, blocks):
    _, near, cap, count = place.shape
    width = blocks[0].shape[1]
    shape = jax.ShapeDtypeStruct((len(ks) * cap, width), jnp.bfloat16)
    return pl.pallas_call(
        lambda *refs: gather_kernel(ks, near, cap, *refs),
        in_specs=[whole_spec(place)] + [whole_spec(block) for block in blocks],
        out_specs=[whole_spec(shape)] * near,
        out_shape=[shape] * near,
        compiler_params=pltpu.CompilerParams(vmem_limit_bytes=MOST_VMEM),
        cost_estimate=pl.CostEstimate(
            flops=2 * len(ks) * near * cap * count * width,
            bytes_accessed=2 * len(ks) * width * (count + near * cap),
            transcendentals=0,
        ),
        name="gather_slots",
    )(place, *blocks)


def combine_kernel(spot_ref, gates_ref, *refs):
    piece_refs, out_ref = refs[:-1], refs[-1]
    total = None
    for d, piece_ref in enumerate(piece_refs):
        weight = spot_ref[0, d].astype(jnp.float32) * gates_ref[0][:, d : d + 1]
        high = weight.astype(jnp.bfloat16)
        for term in (high, (weight - high.astype(jnp.float32)).astype(jnp.bfloat16)):
            part = jnp.dot(term, piece_ref[...], preferred_element_type=jnp.float32)
            total = part if total is None else total + part
    out_ref[...] = total.astype(out_ref.dtype)


def combine_slots(spot, k, i, pieces, dtype, gates):
    _, near, count, cap = spot.shape
    width = pieces[0].shape[1]
    return pl.pallas_call(
        combine_kernel,
        grid=(width // WIDE,),
        in_specs=[
            pl.BlockSpec((1, near, count, cap), lambda j: (k, 0, 0, 0)),
            pl.BlockSpec((1, count, near), lambda j: (k, 0, 0)),
        ]
        + [pl.BlockSpec((cap, WIDE), lambda j: (i, j))] * near,
        out_specs=pl.BlockSpec((count, WIDE), lambda j: (0, j)),
        out_shape=jax.ShapeDtypeStruct((count, width), dtype),
        cost_estimate=pl.CostEstimate(
            flops=4 * near * cap * count * width,
            bytes_accessed=2 * width * (count + near * cap) + 2 * near * cap * count,
            transcendentals=0,
        ),
        name="combine_slots",
    )(spot, gates, *pieces)


class Place:
    def __init__(self, nf, nz):
        self.f, e = lax.axis_index("fsdp"), lax.axis_index("expert")
        self.z, self.c = e // 2, e % 2
        self.nf, self.nz = nf, nz

    def plane(self, k):
        return {"fsdp": self.f, "expert": lax.rem(self.z + k, self.nz) * 2 + self.c}

    def peer(self, d):
        df, dc = d // 2, d % 2
        core = 1 - self.c if dc else self.c
        return {"fsdp": self.flip(df), "expert": self.z * 2 + core}

    def flip(self, df):
        other, bit = 0, 1
        while bit < self.nf:
            digit = lax.rem(self.f // bit, 2)
            other = other + bit * (1 - digit if df & bit else digit)
            bit *= 2
        return other

    def greet(self):
        barrier = pltpu.get_barrier_semaphore()
        others = [self.plane(k) for k in range(1, self.nz)] + [self.peer(d) for d in range(1, 2 * self.nf)]
        for other in others:
            pl.semaphore_signal(barrier, inc=1, device_id=other, device_id_type=MESH)
        pl.semaphore_wait(barrier, len(others))


def remote(source, target, send, recv, device):
    return pltpu.make_async_remote_copy(
        src_ref=source, dst_ref=target, send_sem=send, recv_sem=recv, device_id=device, device_id_type=MESH
    )


def experts_kernel(
    nf, nz, cap, me_ref, place_ref, spot_ref, router_ref, block_ref, wg_any, wu_any, wd_any, *refs
):
    me = Place(nf, nz)
    near = 2 * nf
    early_refs, late_refs, refs = refs[:near], (None, *refs[near : near + nz - 1]), refs[near + nz - 1 :]
    own_ref, arrived_ref, blocks_ref, out_any, act_any, de_any, dgate_any, dup_any, back_ref, parts_ref, cots_ref = refs[:11]
    held, out, rows, cot, wg, wu, wd, de, act, dgate, dup, result, back, part, late, cot_out = refs[11:27]
    z_send, z_recv, sent, got, r_sent, r_got, p_send, p_recv, keep, loads, cot_loads, w_loads, stores, c_sent, c_got = refs[27:]
    width = rows.shape[1]
    tile = 256

    order = [*range(1, nz), 0]
    place_in = {k: i for i, k in enumerate(order)}

    def at(d):
        return pl.ds(d * cap, cap)

    def slot(k):
        return place_in[k] % 2

    def earlier(k, steps):
        return order[place_in[k] - steps] if place_in[k] >= steps else None

    def move(k):
        return remote(block_ref, held.at[k], z_send.at[k], z_recv.at[k], me.plane(k))

    def hop(k, d):
        there = arrived_ref.at[k, at(d)]
        if d == 0:
            return pltpu.make_async_copy(out.at[slot(k), at(d)], there, got.at[k, d])
        return remote(out.at[slot(k), at(d)], there, sent.at[k, d], got.at[k, d], me.peer(d))

    def hop_cot(k, d):
        there = cots_ref.at[k - 1, at(d)]
        if d == 0:
            return pltpu.make_async_copy(cot_out.at[slot(k), at(d)], there, c_got.at[k, d])
        return remote(cot_out.at[slot(k), at(d)], there, c_sent.at[k, d], c_got.at[k, d], me.peer(d))

    def load_cot(k):
        return pltpu.make_async_copy(late_refs[k], late, cot_loads.at[k, 0])

    def hop_back(k, d):
        there = back_ref.at[k, at(d)]
        if d == 0:
            return pltpu.make_async_copy(back.at[slot(k), at(d)], there, r_got.at[k, d])
        return remote(back.at[slot(k), at(d)], there, r_sent.at[k, d], r_got.at[k, d], me.peer(d))

    def along(k):
        return remote(
            part.at[k % 2], parts_ref.at[k - 1], p_send.at[k - 1], p_recv.at[k - 1], me.plane(nz - k)
        )

    def keep_block(k):
        return pltpu.make_async_copy(held.at[k], blocks_ref.at[k], keep.at[k])

    weights = [
        pltpu.make_async_copy(source.at[0], target, w_loads.at[i])
        for i, (source, target) in enumerate(((wg_any, wg), (wu_any, wu), (wd_any, wd)))
    ]
    own = pltpu.make_async_copy(block_ref, held.at[0], z_recv.at[0])

    def saves(k):
        pairs = ((result, out_any), (act, act_any), (de, de_any), (dgate, dgate_any), (dup, dup_any))
        return [pltpu.make_async_copy(source, target.at[k], stores.at[k, i]) for i, (source, target) in enumerate(pairs)]

    def gather(k):
        if k:
            move(k).wait_recv()
        else:
            own.wait()
        keep_block(k).start()
        if earlier(k, 2) is not None:
            for d in range(1, near):
                hop(earlier(k, 2), d).wait_send()
        for d in range(near):
            out[slot(k), at(d)] = jnp.dot(place_ref[k, d], held[k], preferred_element_type=jnp.float32).astype(
                jnp.bfloat16
            )
        for d in range(1, near):
            hop(k, d).start()
        hop(k, 0).start()

    def gather_cot(k):
        load_cot(k).wait()
        if k > 2:
            for d in range(1, near):
                hop_cot(k - 2, d).wait_send()
        for d in range(near):
            cot_out[slot(k), at(d)] = jnp.dot(place_ref[k, d], late[...], preferred_element_type=jnp.float32).astype(
                jnp.bfloat16
            )
        for d in range(1, near):
            hop_cot(k, d).start()
        hop_cot(k, 0).start()
        if k + 1 < nz:
            load_cot(k + 1).start()

    def expert(k):
        for d in range(near):
            hop(k, d).wait() if d == 0 else hop(k, d).wait_recv()
        load = pltpu.make_async_copy(arrived_ref.at[k], rows, loads.at[k])
        load.start()
        if k:
            for d in range(near):
                hop_cot(k, d).wait() if d == 0 else hop_cot(k, d).wait_recv()
            cot_moves = [
                pltpu.make_async_copy(cots_ref.at[k - 1], cot.at[:, pl.ds(0, late.shape[1])], cot_loads.at[k, 1])
            ]
        else:
            cot_moves = [
                pltpu.make_async_copy(early_refs[d], cot.at[at(d), pl.ds(0, late.shape[1])], cot_loads.at[0, d])
                for d in range(near)
            ]
        for one in cot_moves:
            one.start()
        if earlier(k, 1) is not None:
            for one in saves(earlier(k, 1)):
                one.wait()
        else:
            for one in weights:
                one.wait()
        load.wait()
        for one in cot_moves:
            one.wait()
        for d in range(near):
            span = at(d)
            logits = jnp.dot(rows[span, :], router_ref[...], preferred_element_type=jnp.float32)
            picked = cot[span, width : width + logits.shape[1]].astype(jnp.float32) > 0.5
            highest = jnp.max(jnp.where(picked, logits, NEG), axis=-1, keepdims=True)
            raised = jnp.exp(jnp.where(picked, logits - highest, NEG))
            lane = lax.broadcasted_iota(jnp.int32, logits.shape, 1)
            mine = jnp.sum(jnp.where(lane == me_ref[0], raised, 0.0), axis=-1, keepdims=True)
            gate = mine / jnp.maximum(jnp.sum(raised, axis=-1, keepdims=True), 1e-30)
            de[span, :] = (gate * cot[span, :width].astype(jnp.float32)).astype(jnp.bfloat16)

        def hidden(j, _):
            cols = pl.ds(pl.multiple_of(j * tile, tile), tile)
            gate_pre = jnp.dot(rows[...], wg[:, cols], preferred_element_type=jnp.float32)
            up_pre = jnp.dot(rows[...], wu[:, cols], preferred_element_type=jnp.float32)
            sigma = jax.nn.sigmoid(gate_pre)
            act[:, cols] = (gate_pre * sigma * up_pre).astype(jnp.bfloat16)
            d_act = right_product(de[...], wd[cols, :])
            dgate[:, cols] = (d_act * up_pre * sigma * (1.0 + gate_pre * (1.0 - sigma))).astype(jnp.bfloat16)
            dup[:, cols] = (d_act * gate_pre * sigma).astype(jnp.bfloat16)
            return 0

        lax.fori_loop(0, act.shape[1] // tile, hidden, 0)
        if earlier(k, 2) is not None:
            for d in range(1, near):
                hop_back(earlier(k, 2), d).wait_send()

        def model(n, rest):
            cols = pl.ds(pl.multiple_of(n * tile, tile), tile)
            result[:, cols] = jnp.dot(act[...], wd[:, cols], preferred_element_type=jnp.float32).astype(jnp.bfloat16)
            d_rows = right_product(dgate[...], wg[cols, :]) + right_product(dup[...], wu[cols, :])
            back[slot(k), :, cols] = d_rows.astype(jnp.bfloat16)
            return rest + jnp.sum(
                cot[:, cols].astype(jnp.float32) * result[:, cols].astype(jnp.float32), axis=-1, keepdims=True
            )

        rest = lax.fori_loop(0, width // tile, model, jnp.zeros((near * cap, 1), jnp.float32))
        shape = (near * cap, back.shape[2] - width)
        lane = lax.broadcasted_iota(jnp.int32, shape, 1) - (lax.broadcasted_iota(jnp.int32, shape, 0) // cap + k * near) * 3
        extra = jnp.zeros(shape, jnp.float32)
        for i in range(3):
            term = rest.astype(jnp.bfloat16).astype(jnp.float32)
            extra = jnp.where(lane == i, term, extra)
            rest = rest - term
        back[slot(k), :, width:] = extra.astype(jnp.bfloat16)
        for d in range(1, near):
            hop_back(k, d).start()
        hop_back(k, 0).start()
        for one in saves(k):
            one.start()

    def combine(k):
        for d in range(near):
            hop_back(k, d).wait() if d == 0 else hop_back(k, d).wait_recv()
        load = pltpu.make_async_copy(back_ref.at[k], cot.at[:, pl.ds(0, back.shape[2])], loads.at[nz + k])
        load.start()
        load.wait()
        for d in range(near):
            term = jnp.dot(spot_ref[k, d], cot[at(d), : back.shape[2]], preferred_element_type=jnp.float32)
            if d:
                own_ref[...] += term
            else:
                own_ref[...] = term
        if k:
            if k > 2:
                along(k - 2).wait_send()
            part[k % 2] = own_ref[...].astype(jnp.bfloat16)
            along(k).start()

    for one in weights:
        one.start()
    me.greet()
    for k in range(1, nz):
        move(k).start()
    own.start()
    load_cot(1).start()
    gather_cot(1)
    gather(1)
    for k in range(1, nz):
        if k + 1 < nz:
            gather_cot(k + 1)
        if k == 1:
            expert(k)
        if k + 1 < nz:
            gather(k + 1)
        else:
            gather(0)
        if k > 1:
            combine(k - 1)
            expert(k)
    combine(nz - 1)
    expert(0)
    combine(0)
    for k in range(nz):
        keep_block(k).wait()
        if k:
            move(k).wait_send()
            if k >= nz - 2:
                along(k).wait_send()
            along(k).wait_recv()
    for k in order[-2:]:
        for d in range(1, near):
            hop(k, d).wait_send()
            hop_back(k, d).wait_send()
    for k in (nz - 2, nz - 1):
        for d in range(1, near):
            hop_cot(k, d).wait_send()
    for one in saves(order[-1]):
        one.wait()


def run_experts(nf, me, place, spot, router, block, w_gate, w_up, w_down, early, late):
    nz, near, cap, count = place.shape
    width, hidden = w_gate.shape[1:]
    rows = near * cap
    extra = -(-3 * near * nz // 128) * 128
    wide = max(width + extra, early[0].shape[1])
    low = jnp.bfloat16
    anywhere = pl.BlockSpec(memory_space=pl.ANY)
    own = jax.ShapeDtypeStruct((count, width + extra), jnp.float32)
    shapes = [
        jax.ShapeDtypeStruct(shape, low)
        for shape in (
            (nz, rows, width),
            (nz, count, width),
            (nz, rows, width),
            (nz, rows, hidden),
            (nz, rows, width),
            (nz, rows, hidden),
            (nz, rows, hidden),
            (nz, rows, width + extra),
            (nz - 1, count, width + extra),
            (nz - 1, rows, early[0].shape[1]),
        )
    ]
    dma = pltpu.SemaphoreType.DMA
    return pl.pallas_call(
        lambda *refs: experts_kernel(nf, nz, cap, *refs),
        in_specs=[SCALARS, whole_spec(place), whole_spec(spot), whole_spec(router)] + [anywhere] * (4 + near + len(late)),
        out_specs=[whole_spec(own)] + [anywhere] * len(shapes),
        out_shape=[own] + shapes,
        scratch_shapes=[
            pltpu.VMEM((nz, count, width), low),
            pltpu.VMEM((2, rows, width), low),
            pltpu.VMEM((rows, width), low),
            pltpu.VMEM((rows, wide), low),
            pltpu.VMEM((width, hidden), low),
            pltpu.VMEM((width, hidden), low),
            pltpu.VMEM((hidden, width), low),
            pltpu.VMEM((rows, width), low),
            pltpu.VMEM((rows, hidden), low),
            pltpu.VMEM((rows, hidden), low),
            pltpu.VMEM((rows, hidden), low),
            pltpu.VMEM((rows, width), low),
            pltpu.VMEM((2, rows, width + extra), low),
            pltpu.VMEM((2, count, width + extra), low),
            pltpu.VMEM((count, early[0].shape[1]), low),
            pltpu.VMEM((2, rows, early[0].shape[1]), low),
            dma((nz,)),
            dma((nz,)),
            dma((nz, near)),
            dma((nz, near)),
            dma((nz, near)),
            dma((nz, near)),
            dma((nz - 1,)),
            dma((nz - 1,)),
            dma((nz,)),
            dma((2 * nz,)),
            dma((nz, near)),
            dma((3,)),
            dma((nz, 5)),
            dma((nz, near)),
            dma((nz, near)),
        ],
        compiler_params=pltpu.CompilerParams(collective_id=0, has_side_effects=True, vmem_limit_bytes=MOST_VMEM),
        cost_estimate=pl.CostEstimate(
            flops=12 * nz * rows * width * hidden, bytes_accessed=600_000_000, transcendentals=0
        ),
        name="run_experts",
    )(me, place, spot, router, block, w_gate, w_up, w_down, *early, *late)


def whole_spec(value):
    return pl.BlockSpec(value.shape, lambda *_: (0,) * len(value.shape))


SCALARS = pl.BlockSpec(memory_space=pltpu.SMEM)


def scores_of(q_rot, k_rot, seg_col, seg_row):
    scores = right_product(q_rot, k_rot) * HEAD_SIZE ** (-0.5)
    here = lax.broadcasted_iota(jnp.int32, scores.shape, 0) >= lax.broadcasted_iota(jnp.int32, scores.shape, 1)
    return jnp.where(here & (seg_col == seg_row), scores, NEG)


def turn(value, cos, sin):
    return value * cos + pltpu.roll(value, HEAD_SIZE // 2, 1) * sin


def attend_kernel(blocks, heads, kv_heads, spots, x_ref, gain_ref, row_ref, col_ref, cos_ref, sin_ref, qg_ref, kg_ref, *refs):
    w_refs, refs = refs[:blocks], refs[blocks:]
    normed_ref, raw_ref, rot_ref, value_ref, mixed_ref, lse_ref = refs
    wide = x_ref[...].astype(jnp.float32)
    normed_ref[...] = (wide * inverse_norm(wide) * gain_ref[...]).astype(jnp.bfloat16)
    depth = w_refs[0].shape[0]
    total = None
    for i, w_ref in enumerate(w_refs):
        part = normed_ref[...] if blocks == 1 else normed_ref[:, pl.ds(pl.multiple_of(spots[i] * depth, depth), depth)]
        part = jnp.dot(part, w_ref[...], preferred_element_type=jnp.float32)
        total = part if total is None else total + part
    turned = (heads + kv_heads) * HEAD_SIZE
    raw_ref[...] = total[:, :turned]
    value_ref[...] = total[:, turned:].astype(jnp.bfloat16)
    cos, sin = cos_ref[...], sin_ref[...]
    for h in range(heads + kv_heads):
        at = slice(h * HEAD_SIZE, (h + 1) * HEAD_SIZE)
        raw = raw_ref[:, at]
        gain = qg_ref[...] if h < heads else kg_ref[...]
        rot_ref[:, at] = turn(raw * inverse_norm(raw) * gain, cos, sin).astype(jnp.bfloat16)
    lane = lax.broadcasted_iota(jnp.int32, lse_ref.shape, 1)
    all_lse = jnp.zeros(lse_ref.shape, jnp.float32)
    for h in range(heads):
        at = slice(h * HEAD_SIZE, (h + 1) * HEAD_SIZE)
        g = h * kv_heads // heads
        masked = scores_of(
            rot_ref[:, at],
            rot_ref[:, (heads + g) * HEAD_SIZE : (heads + g + 1) * HEAD_SIZE],
            col_ref[...],
            row_ref[...],
        )
        top = jnp.max(masked, axis=-1, keepdims=True)
        lse = top + jnp.log(jnp.sum(jnp.exp(masked - top), axis=-1, keepdims=True))
        prob_low = jnp.exp(masked - lse).astype(jnp.bfloat16)
        mixed_ref[:, at] = jnp.dot(
            prob_low, value_ref[:, g * HEAD_SIZE : (g + 1) * HEAD_SIZE], preferred_element_type=jnp.float32
        ).astype(jnp.bfloat16)
        all_lse = jnp.where(lane == h, lse, all_lse)
    lse_ref[...] = all_lse


def attend(spots, tokens, gain, seg_row, seg_col, cos, sin, qg, kg, w_blocks, heads, kv_heads):
    count, width = tokens.shape
    args = (tokens, gain, seg_row, seg_col, cos, sin, qg, kg, *w_blocks)
    shapes = [
        jax.ShapeDtypeStruct((count, width), jnp.bfloat16),
        jax.ShapeDtypeStruct((count, (heads + kv_heads) * HEAD_SIZE), jnp.float32),
        jax.ShapeDtypeStruct((count, (heads + kv_heads) * HEAD_SIZE), jnp.bfloat16),
        jax.ShapeDtypeStruct((count, kv_heads * HEAD_SIZE), jnp.bfloat16),
        jax.ShapeDtypeStruct((count, heads * HEAD_SIZE), jnp.bfloat16),
        jax.ShapeDtypeStruct((count, 128), jnp.float32),
    ]
    return pl.pallas_call(
        lambda *refs: attend_kernel(len(w_blocks), heads, kv_heads, *refs),
        in_specs=[SCALARS] + [whole_spec(v) for v in args],
        out_specs=[whole_spec(v) for v in shapes],
        out_shape=shapes,
        cost_estimate=pl.CostEstimate(
            flops=2 * count * width * (heads + 2 * kv_heads) * HEAD_SIZE + 4 * heads * count * count * HEAD_SIZE,
            bytes_accessed=2 * width * (heads + 2 * kv_heads) * HEAD_SIZE + 16 * count * width,
            transcendentals=2 * heads * count * count,
        ),
        name="attend",
    )(spots, *args)


def project_kernel(blocks, spots, mixed_ref, *refs):
    w_refs, out_ref = refs[:blocks], refs[-1]
    depth = w_refs[0].shape[0]
    total = None
    for i, w_ref in enumerate(w_refs):
        part = mixed_ref[...] if blocks == 1 else mixed_ref[:, pl.ds(pl.multiple_of(spots[i] * depth, depth), depth)]
        part = jnp.dot(part, w_ref[...], preferred_element_type=jnp.float32)
        total = part if total is None else total + part
    out_ref[...] = total.astype(out_ref.dtype)


def project(spots, mixed, w_blocks, dtype):
    count, depth = mixed.shape
    width = w_blocks[0].shape[1]
    return pl.pallas_call(
        lambda *refs: project_kernel(len(w_blocks), *refs),
        grid=(width // WIDE,),
        in_specs=[SCALARS, pl.BlockSpec((count, depth), lambda j: (0, 0))]
        + [pl.BlockSpec((w.shape[0], WIDE), lambda j: (0, j)) for w in w_blocks],
        out_specs=pl.BlockSpec((count, WIDE), lambda j: (0, j)),
        out_shape=jax.ShapeDtypeStruct((count, width), dtype),
        cost_estimate=pl.CostEstimate(
            flops=2 * count * depth * width, bytes_accessed=2 * depth * width + 4 * count * width, transcendentals=0
        ),
        name="project",
    )(spots, mixed, *w_blocks)


def head_back(grad_rot, raw, gain, cos, sin):
    grad_normed = turn(grad_rot, cos, -sin)
    rinv = inverse_norm(raw)
    gain_grad = jnp.sum(grad_normed * raw * rinv, axis=0, keepdims=True)
    scaled = grad_normed * gain
    return rinv * scaled - raw * rinv**3 * jnp.mean(scaled * raw, axis=-1, keepdims=True), gain_grad


def attend_back_kernel(
    blocks, heads, kv_heads, spots, dmid_ref, x_ref, row_ref, col_ref, cos_ref, sin_ref, qg_ref, kg_ref,
    raw_ref, rot_ref, value_ref, mixed_ref, lse_ref, *refs
):
    o_refs, w_refs, refs = refs[:blocks], refs[blocks : 2 * blocks], refs[2 * blocks :]
    dheads_ref, part_ref, gain_ref, qgain_ref, kgain_ref, dmixed = refs
    scale = HEAD_SIZE ** (-0.5)
    dmid = dmid_ref[...]
    depth = o_refs[0].shape[0]
    for i, o_ref in enumerate(o_refs):
        part = right_product(dmid, o_ref[...]).astype(jnp.bfloat16)
        if blocks == 1:
            dmixed[...] = part
        else:
            dmixed[:, pl.ds(pl.multiple_of(spots[i] * depth, depth), depth)] = part
    cos, sin = cos_ref[...], sin_ref[...]
    lane = lax.broadcasted_iota(jnp.int32, lse_ref.shape, 1)
    all_lse = lse_ref[...]
    q_gain = jnp.zeros(qgain_ref.shape, jnp.float32)
    k_gain = jnp.zeros(kgain_ref.shape, jnp.float32)
    for g in range(kv_heads):
        kv = slice(g * HEAD_SIZE, (g + 1) * HEAD_SIZE)
        key_at = slice((heads + g) * HEAD_SIZE, (heads + g + 1) * HEAD_SIZE)
        k_rot, value = rot_ref[:, key_at], value_ref[:, kv]
        d_value, d_key = None, None
        for h in range(g * heads // kv_heads, (g + 1) * heads // kv_heads):
            at = slice(h * HEAD_SIZE, (h + 1) * HEAD_SIZE)
            q_rot, grad = rot_ref[:, at], dmixed[:, at]
            lse = jnp.sum(jnp.where(lane == h, all_lse, 0.0), axis=-1, keepdims=True)
            prob = jnp.exp(scores_of(q_rot, k_rot, col_ref[...], row_ref[...]) - lse)
            part = left_product(prob.astype(jnp.bfloat16), grad)
            d_value = part if d_value is None else d_value + part
            d_prob = right_product(grad, value)
            delta = jnp.sum(grad.astype(jnp.float32) * mixed_ref[:, at].astype(jnp.float32), axis=-1, keepdims=True)
            d_scores = (prob * (d_prob - delta)).astype(jnp.bfloat16)
            part = left_product(d_scores, q_rot)
            d_key = part if d_key is None else d_key + part
            d_q = jnp.dot(d_scores, k_rot, preferred_element_type=jnp.float32) * scale
            d_query, gain_part = head_back(d_q, raw_ref[:, at], qg_ref[...], cos, sin)
            q_gain = q_gain + gain_part
            dheads_ref[:, at] = d_query.astype(jnp.bfloat16)
        d_key, gain_part = head_back(d_key * scale, raw_ref[:, key_at], kg_ref[...], cos, sin)
        k_gain = k_gain + gain_part
        dheads_ref[:, key_at] = d_key.astype(jnp.bfloat16)
        last = (heads + kv_heads + g) * HEAD_SIZE
        dheads_ref[:, last : last + HEAD_SIZE] = d_value.astype(jnp.bfloat16)
    qgain_ref[...] = q_gain
    kgain_ref[...] = k_gain
    d_heads = dheads_ref[...]
    wide = x_ref[...].astype(jnp.float32)
    rinv = inverse_norm(wide)
    depth = w_refs[0].shape[0]
    for i, w_ref in enumerate(w_refs):
        part = right_product(d_heads, w_ref[...])
        at = slice(None) if blocks == 1 else pl.ds(pl.multiple_of(spots[i] * depth, depth), depth)
        part_ref[:, at] = part.astype(part_ref.dtype)
        x = x_ref[:, at].astype(jnp.float32)
        gain_ref[:, at] = jnp.sum(part * x * rinv, axis=0, keepdims=True)


def attend_back(spots, dmid, tokens, seg_row, seg_col, cos, sin, qg, kg, saved, o_blocks, w_blocks, heads, kv_heads, dtype):
    count, width = tokens.shape
    args = (dmid, tokens, seg_row, seg_col, cos, sin, qg, kg, *saved, *o_blocks, *w_blocks)
    lanes = (heads + 2 * kv_heads) * HEAD_SIZE
    shapes = [
        jax.ShapeDtypeStruct((count, lanes), jnp.bfloat16),
        jax.ShapeDtypeStruct((count, width), dtype),
        jax.ShapeDtypeStruct((1, width), jnp.float32),
        jax.ShapeDtypeStruct((1, HEAD_SIZE), jnp.float32),
        jax.ShapeDtypeStruct((1, HEAD_SIZE), jnp.float32),
    ]
    return pl.pallas_call(
        lambda *refs: attend_back_kernel(len(w_blocks), heads, kv_heads, *refs),
        in_specs=[SCALARS] + [whole_spec(v) for v in args],
        out_specs=[whole_spec(v) for v in shapes],
        out_shape=shapes,
        scratch_shapes=[pltpu.VMEM((count, heads * HEAD_SIZE), jnp.bfloat16)],
        cost_estimate=pl.CostEstimate(
            flops=4 * count * width * lanes + 10 * heads * count * count * HEAD_SIZE,
            bytes_accessed=4 * width * lanes + 24 * count * width,
            transcendentals=heads * count * count,
        ),
        name="attend_back",
    )(spots, *args)


def on_device(
    tokens,
    segments,
    routes,
    attn_gain,
    w_query,
    key_matrix,
    value_matrix,
    output_matrix,
    query_gain,
    key_gain,
    ffn_gain,
    w_router,
    w_gate,
    w_up,
    w_down,
    cotangent,
):
    nf, ne = lax.axis_size("fsdp"), lax.axis_size("expert")
    nz = ne // 2
    f, e = lax.axis_index("fsdp"), lax.axis_index("expert")
    z, c = e // 2, e % 2
    count = tokens.shape[0]
    experts = nf * ne
    cap = -(5 * count * TOP // (4 * experts)) // 16 * -16
    peers = [(df, dc) for df in range(nf) for dc in range(2)]
    near = len(peers)

    def across(value, df, dc):
        return lax.ppermute(
            value, ALL, [(i * ne + j, (i ^ df) * ne + (j ^ dc)) for i in range(nf) for j in range(ne)]
        )

    def along(value, k):
        return lax.ppermute(value, "expert", [(j, (j + 2 * k) % ne) for j in range(ne)])

    def group_blocks(value):
        return [value] + [across(value, df, 0) for df in range(1, nf)]

    def plane_blocks(value):
        blocks = [value]
        for k in range(1, nz):
            blocks.append(along(value, k))
        return blocks

    def spread_rows(blocks):
        rows, width = blocks[0].shape
        places, pieces = [], []
        for k, block in enumerate(blocks):
            places += [(z - k) % nz * 2 + c, (z - k) % nz * 2 + 1 - c]
            pieces += [block, across(block, 0, 1)]
        if rows % 128 == 0:
            return pieces, jnp.stack(places).astype(jnp.int32)
        whole = jnp.zeros((ne, rows, width), blocks[0].dtype)
        for at, piece in zip(places, pieces):
            whole = lax.dynamic_update_slice(whole, piece[None], (at, 0, 0))
        return [whole.reshape(ne * rows, width)], jnp.zeros((1,), jnp.int32)

    def reduce_rows(grad):
        grad = grad.reshape(nz, 2, grad.shape[0] // ne, grad.shape[1])
        theirs = lax.dynamic_index_in_dim(grad, 1 - c, 1, keepdims=False).astype(jnp.bfloat16)
        mine = lax.dynamic_index_in_dim(grad, c, 1, keepdims=False)
        mine = mine + across(theirs, 0, 1).astype(jnp.float32)
        total = lax.dynamic_index_in_dim(mine, z, 0, keepdims=False)
        parts = [lax.dynamic_index_in_dim(mine, (z + k) % nz, 0, keepdims=False) for k in range(1, nz)]
        parts = [part.astype(jnp.bfloat16) for part in parts]
        for k, part in enumerate(parts, 1):
            total = total + along(part, k).astype(jnp.float32)
        return total, parts

    def add_pairs(values):
        while len(values) > 1:
            values = [a + b for a, b in zip(values[::2], values[1::2])]
        return values[0]

    def sum_small(columns, row, *earlier):
        blocks = columns.reshape(nz, 2, MODEL_WIDTH // ne, columns.shape[1])
        rows = jnp.broadcast_to(row[None, None], (nz, 2) + row.shape)
        blocks = jnp.concatenate([blocks, rows], axis=2)
        mine = lax.dynamic_index_in_dim(blocks, c, 1, keepdims=False)
        mine = mine + across(lax.dynamic_index_in_dim(blocks, 1 - c, 1, keepdims=False), 0, 1)
        mine = after(mine, *earlier)
        sends = [lax.dynamic_index_in_dim(mine, z ^ step, 0, keepdims=False) for step in range(nz)]
        pairs = [[(j, j ^ (2 * step)) for j in range(ne)] for step in range(nz)]
        return add_pairs([lax.ppermute(v, "expert", p) if i else v for i, (v, p) in enumerate(zip(sends, pairs))])

    width_q, width_k = w_query.shape[1], key_matrix.shape[1]
    w_heads = jnp.concatenate([w_query, key_matrix, value_matrix], axis=1)
    token_blocks = group_blocks(tokens)
    segment_blocks = group_blocks(segments)
    few = jnp.concatenate(
        [jnp.transpose(routes).astype(jnp.bfloat16).reshape(-1, w_router.shape[0]), attn_gain[None], ffn_gain[None], jnp.transpose(w_router)]
    )
    few_blocks = plane_blocks(few)
    heads_blocks = plane_blocks(after(w_heads, few))
    few_pairs = across(jnp.stack([block[-experts - 2 :] for block in few_blocks]), 0, 1)
    few_whole = jnp.zeros((nz, 2) + few_pairs.shape[1:], jnp.bfloat16)
    for k, block in enumerate(few_blocks):
        for core, piece in ((c, block[-experts - 2 :]), (1 - c, few_pairs[k])):
            few_whole = lax.dynamic_update_slice(few_whole, piece[None, None], ((z - k) % nz, core, 0, 0))
    few_whole = jnp.transpose(few_whole, (2, 0, 1, 3)).reshape(experts + 2, MODEL_WIDTH)
    gain_one, gain_two = few_whole[:1].astype(jnp.float32), few_whole[1:2].astype(jnp.float32)
    full_router = jnp.transpose(jnp.pad(few_whole[2:], ((0, -experts % 128), (0, 0))))
    route_blocks = [block[: -experts - 2].reshape(TOP, count).astype(jnp.int32) for block in few_blocks]
    picked = jnp.any(routes[:, :, None] == jnp.arange(full_router.shape[1])[None, None, :], axis=1)
    cot_wide = jnp.concatenate([cotangent, picked.astype(jnp.bfloat16)], axis=1)

    peer_experts = jnp.stack([(f ^ df) * ne + 2 * z + (c ^ dc) for df, dc in peers])
    named = jnp.stack(route_blocks)
    hit = jnp.any(named[:, None] == peer_experts[None, :, None, None], axis=2)
    upto = (jnp.arange(count)[:, None] <= jnp.arange(count)[None, :]).astype(jnp.bfloat16)
    rank = jnp.dot(
        hit.astype(jnp.bfloat16).reshape(nz * near, count), upto, preferred_element_type=jnp.float32
    ).reshape(nz, near, count)
    slot_of = jnp.where(hit, rank - 1.0, -1.0)
    slots = jnp.arange(cap, dtype=jnp.float32)
    place = (slot_of[:, :, None, :] == slots[None, None, :, None]).astype(jnp.bfloat16)
    spot = (slot_of[:, :, :, None] == slots[None, None, None, :]).astype(jnp.bfloat16)

    def send_out(pieces):
        got = [pieces[0]]
        for d, (df, dc) in enumerate(peers[1:], 1):
            got.append(across(pieces[d], df, dc))
        return got

    early = send_out(gather_slots(place, (0,), [after(cot_wide, *token_blocks[1:])]))

    local_q = width_q // HEAD_SIZE
    local_kv = width_k // HEAD_SIZE
    w_blocks, spots = spread_rows([after(block, few_whole) for block in heads_blocks])
    head_blocks = plane_blocks(after(output_matrix, *w_blocks))
    cot_blocks = plane_blocks(after(cot_wide, *w_blocks))
    cosine, sine = rotary_tables(SEQ, HEAD_SIZE)
    cos = jnp.concatenate([cosine[0, :, 0], cosine[0, :, 0]], axis=-1)
    sin = jnp.concatenate([-sine[0, :, 0], sine[0, :, 0]], axis=-1)
    q_scale = query_gain.astype(jnp.float32)[None]
    k_scale = key_gain.astype(jnp.float32)[None]
    turns = [1 + df for df in range(nf - 1)] + [0]
    shared = [
        (segment_blocks[df], jnp.transpose(segment_blocks[df]), cos, sin, q_scale, k_scale) for df in range(nf)
    ]
    attended = [None] * nf
    for turn_at, df in enumerate(turns):
        attended[df] = attend(
            spots,
            after(token_blocks[df], *([attended[turns[turn_at - 1]][4]] if turn_at else [])),
            gain_one,
            *shared[df],
            w_blocks,
            local_q,
            local_kv,
        )
    o_blocks, _ = spread_rows([after(block, attended[turns[-2]][0]) for block in head_blocks])
    wide_in = tokens.astype(jnp.float32)
    rinv_one = inverse_norm(wide_in)
    residual_mid = wide_in
    for df in turns:
        part = project(spots, attended[df][4], o_blocks, jnp.bfloat16 if df else jnp.float32)
        if df:
            part = across(part, df, 0).astype(jnp.float32)
        residual_mid = residual_mid + part

    rinv_two = inverse_norm(residual_mid)
    normed_two = (residual_mid * rinv_two * gain_two).astype(jnp.bfloat16)
    me = (f * ne + e).astype(jnp.int32)[None]
    own_sum, arrived, normed_blocks, expert_out, act, d_expert, d_gate_pre, d_up_pre, _, plane_sums, _ = run_experts(
        nf, me, place, spot, full_router, normed_two, w_gate, w_up, w_down, early, cot_blocks[1:]
    )
    back_sum = own_sum + jnp.sum(plane_sums.astype(jnp.float32), axis=0)
    d_normed_two = back_sum[:, :MODEL_WIDTH]

    def gates_of(rows, named_rows):
        logits = jnp.dot(rows, full_router, preferred_element_type=jnp.float32)[:, :experts]
        picked = jnp.any(named_rows[:, :, None] == jnp.arange(experts)[None, None, :], axis=0)
        highest = jnp.max(jnp.where(picked, logits, NEG), axis=-1, keepdims=True)
        raised = jnp.where(picked, jnp.exp(jnp.minimum(logits - highest, 0.0)), 0.0)
        return raised / jnp.sum(raised, axis=-1, keepdims=True)

    gates = gates_of(normed_two, route_blocks[0])

    owners = jnp.concatenate(
        [jnp.repeat(peer_experts + 2 * ((z + k) % nz - z), 3) for k in range(nz)]
    )
    names = (owners[:, None] == jnp.arange(experts)[None, :]).astype(jnp.float32)
    d_gates = jnp.dot(
        back_sum[:, MODEL_WIDTH : MODEL_WIDTH + 3 * near * nz], names, precision=lax.Precision.HIGHEST
    )
    d_logits = (gates * (d_gates - jnp.sum(gates * d_gates, axis=-1, keepdims=True))).astype(jnp.bfloat16)

    router_grad = left_product(normed_two, d_logits)
    d_normed_two = d_normed_two + right_product(d_logits, full_router[:, :experts])
    d_norm_part, gain_two_grad = row_norm_back(d_normed_two, residual_mid, rinv_two, gain_two)
    d_mid = cotangent.astype(jnp.float32) + d_norm_part
    middle_blocks = group_blocks(d_mid.astype(jnp.bfloat16))
    arrived, act, d_expert, d_gate_pre, d_up_pre = after(
        tuple(
            value.reshape(nz * near * cap, value.shape[2])
            for value in (arrived, act, d_expert, d_gate_pre, d_up_pre)
        ),
        middle_blocks[0],
    )
    down_grad = left_product(act, d_expert)
    gate_grad = left_product(arrived, d_gate_pre)
    up_grad = left_product(arrived, d_up_pre)

    is_peer = peer_experts[None, :, None] == jnp.arange(experts)[None, None, :]
    peer_gates = jnp.stack(
        [
            jnp.sum(jnp.where(is_peer, gates_of(normed_blocks[k], route_blocks[k])[:, None, :], 0.0), axis=-1)
            for k in range(nz)
        ]
    )
    expert_out = after(expert_out, *middle_blocks[1:])
    groups = [list(range(1, nz // 2 + 1)), list(range(nz // 2 + 1, nz)) + [0]]
    come = {}
    for group in groups:
        pieces = [
            jnp.concatenate([expert_out[k, d * cap : (d + 1) * cap] for k in group], axis=0) for d in range(near)
        ]
        pieces = send_out(pieces)
        for i, k in enumerate(group):
            come[k] = (i, pieces)

    home_parts = {}

    def home_sum(k, weights):
        part = combine_slots(spot, k, *come[k], jnp.bfloat16 if k else jnp.float32, weights)
        home_parts[k] = part
        if k:
            part = along(part, nz - k).astype(jnp.float32)
        return part

    mixed = jnp.concatenate([attended[df][4] for df in range(nf)], axis=0)
    share_out, out_parts = reduce_rows(left_product(mixed, jnp.concatenate(middle_blocks, axis=0)))
    moe = [home_sum(k, after(peer_gates, *out_parts)) for k in groups[0]]
    d_heads = [None] * nf
    d_normed_one, gain_one_grad, q_gain_grad, k_gain_grad = None, None, None, None
    for df in range(nf):
        d_heads[df], part, *sums = attend_back(
            spots,
            after(
                middle_blocks[df],
                *([d_heads[df - 1]] if df else []),
                *([home_parts[k] for k in groups[0]] if df == nf - 1 else []),
            ),
            token_blocks[df],
            *shared[df],
            attended[df][1:],
            o_blocks,
            w_blocks,
            local_q,
            local_kv,
            jnp.bfloat16 if df else jnp.float32,
        )
        if df:
            part = across(part, df, 0).astype(jnp.float32)
            d_normed_one = d_normed_one + part
            gain_one_grad, q_gain_grad, k_gain_grad = [
                a + b for a, b in zip((gain_one_grad, q_gain_grad, k_gain_grad), sums)
            ]
        else:
            d_normed_one = part
            gain_one_grad, q_gain_grad, k_gain_grad = sums
    normed_one = jnp.concatenate([attended[df][0] for df in range(nf)], axis=0)
    share_heads, head_parts = reduce_rows(left_product(normed_one, jnp.concatenate(d_heads, axis=0)))
    columns = jnp.concatenate([router_grad, jnp.transpose(gain_one_grad), gain_two_grad[:, None]], axis=1)
    columns = jnp.pad(columns, ((0, 0), (0, -columns.shape[1] % 128)))
    row = jnp.pad(jnp.concatenate([q_gain_grad, k_gain_grad]), ((0, 6), (0, columns.shape[1] - HEAD_SIZE)))
    small = sum_small(columns, row, *head_parts)
    for k in groups[1]:
        moe.append(home_sum(k, after(peer_gates, *head_parts)))
    moe = sum(moe[1:], moe[0])
    output = (residual_mid + moe).astype(jnp.bfloat16)
    small = after(small, home_parts[0])
    small = add_pairs([across(small, df, 0) if df else small for df in range(nf)])

    d_tokens, _ = row_norm_back(d_normed_one, wide_in, rinv_one, gain_one)
    token_grad = d_mid + d_tokens

    rows_own = MODEL_WIDTH // ne
    return (
        output,
        token_grad,
        small[:rows_own, experts],
        share_heads[:, :width_q],
        share_heads[:, width_q : width_q + width_k],
        share_heads[:, width_q + width_k :],
        share_out,
        small[rows_own, :HEAD_SIZE],
        small[rows_own + 1, :HEAD_SIZE],
        small[:rows_own, experts + 1],
        small[:rows_own, :experts],
        gate_grad[None],
        up_grad[None],
        down_grad[None],
    )


def solution(mesh):
    return jax.shard_map(
        on_device,
        mesh=mesh,
        in_specs=(
            P(("fsdp", "expert"), None),
            P(("fsdp", "expert"), None),
            P(("fsdp", "expert"), None),
            P("expert"),
            P("expert", "fsdp"),
            P("expert", "fsdp"),
            P("expert", "fsdp"),
            P(("fsdp", "expert"), None),
            P(),
            P(),
            P("expert"),
            P("expert", None),
            P(("fsdp", "expert"), None, None),
            P(("fsdp", "expert"), None, None),
            P(("fsdp", "expert"), None, None),
            P(("fsdp", "expert"), None),
        ),
        out_specs=(
            P(("fsdp", "expert"), None),
            P(("fsdp", "expert"), None),
            P("expert"),
            P("expert", "fsdp"),
            P("expert", "fsdp"),
            P("expert", "fsdp"),
            P(("fsdp", "expert"), None),
            P(),
            P(),
            P("expert"),
            P("expert", None),
            P(("fsdp", "expert"), None, None),
            P(("fsdp", "expert"), None, None),
            P(("fsdp", "expert"), None, None),
        ),
        check_vma=False,
    )
```

```python
import jax
import jax.numpy as jnp
from jax import lax
from jax.experimental import pallas as pl
from jax.experimental.pallas import tpu as pltpu
from jax.sharding import PartitionSpec as P


MODEL_WIDTH = 2048
HEAD_SIZE = 128
TOP = 8
SEQ = 256


EPS = 1e-06
THETA = 1000000.0
NEG = -1e30


def inverse_norm(value):
    return lax.rsqrt(jnp.mean(value * value, axis=-1, keepdims=True) + EPS)


def rotary_tables(sequence_length, width):
    half = width // 2
    inverse = THETA ** (-(jnp.arange(half).astype(jnp.float32) * 2.0 / width))
    angle = jnp.arange(sequence_length).astype(jnp.float32)[:, None] * inverse[None, :]
    return (jnp.cos(angle)[None, :, None, :], jnp.sin(angle)[None, :, None, :])


def row_norm_back(grad_normed, raw, rinv, gain):
    gain_grad = jnp.sum(grad_normed * raw * rinv, axis=0)
    scaled = grad_normed * gain
    grad_raw = rinv * scaled - raw * rinv**3 * jnp.mean(scaled * raw, axis=-1, keepdims=True)
    return (grad_raw, gain_grad)


def left_product(left, right):
    return lax.dot_general(
        left, right, (((0,), (0,)), ((), ())), preferred_element_type=jnp.float32
    )


def right_product(left, right):
    return lax.dot_general(
        left, right, (((1,), (1,)), ((), ())), preferred_element_type=jnp.float32
    )


ALL = ("fsdp", "expert")
WIDE = 512


def after(value, *earlier):
    return lax.optimization_barrier((value, *earlier))[0]


MESH = pl.DeviceIdType.MESH
MOST_VMEM = 62 * 1024 * 1024


def gather_kernel(ks, near, cap, place_ref, *refs):
    block_refs, out_refs = refs[: len(ks)], refs[len(ks) :]
    for i, (k, block_ref) in enumerate(zip(ks, block_refs)):
        for d in range(near):
            out_refs[d][i * cap : (i + 1) * cap, :] = jnp.dot(
                place_ref[k, d], block_ref[...], preferred_element_type=jnp.float32
            ).astype(jnp.bfloat16)


def gather_slots(place, ks, blocks):
    _, near, cap, count = place.shape
    width = blocks[0].shape[1]
    shape = jax.ShapeDtypeStruct((len(ks) * cap, width), jnp.bfloat16)
    return pl.pallas_call(
        lambda *refs: gather_kernel(ks, near, cap, *refs),
        in_specs=[whole_spec(place)] + [whole_spec(block) for block in blocks],
        out_specs=[whole_spec(shape)] * near,
        out_shape=[shape] * near,
        compiler_params=pltpu.CompilerParams(vmem_limit_bytes=MOST_VMEM),
        cost_estimate=pl.CostEstimate(
            flops=2 * len(ks) * near * cap * count * width,
            bytes_accessed=2 * len(ks) * width * (count + near * cap),
            transcendentals=0,
        ),
        name="gather_slots",
    )(place, *blocks)


def combine_kernel(spot_ref, gates_ref, *refs):
    piece_refs, out_ref = refs[:-1], refs[-1]
    total = None
    for d, piece_ref in enumerate(piece_refs):
        weight = spot_ref[0, d].astype(jnp.float32) * gates_ref[0][:, d : d + 1]
        high = weight.astype(jnp.bfloat16)
        for term in (high, (weight - high.astype(jnp.float32)).astype(jnp.bfloat16)):
            part = jnp.dot(term, piece_ref[...], preferred_element_type=jnp.float32)
            total = part if total is None else total + part
    out_ref[...] = total.astype(out_ref.dtype)


def combine_slots(spot, k, i, pieces, dtype, gates):
    _, near, count, cap = spot.shape
    width = pieces[0].shape[1]
    return pl.pallas_call(
        combine_kernel,
        grid=(width // WIDE,),
        in_specs=[
            pl.BlockSpec((1, near, count, cap), lambda j: (k, 0, 0, 0)),
            pl.BlockSpec((1, count, near), lambda j: (k, 0, 0)),
        ]
        + [pl.BlockSpec((cap, WIDE), lambda j: (i, j))] * near,
        out_specs=pl.BlockSpec((count, WIDE), lambda j: (0, j)),
        out_shape=jax.ShapeDtypeStruct((count, width), dtype),
        cost_estimate=pl.CostEstimate(
            flops=4 * near * cap * count * width,
            bytes_accessed=2 * width * (count + near * cap) + 2 * near * cap * count,
            transcendentals=0,
        ),
        name="combine_slots",
    )(spot, gates, *pieces)


class Place:
    def __init__(self, nf, nz):
        self.f, e = lax.axis_index("fsdp"), lax.axis_index("expert")
        self.z, self.c = e // 2, e % 2
        self.nf, self.nz = nf, nz

    def plane(self, k):
        return {"fsdp": self.f, "expert": lax.rem(self.z + k, self.nz) * 2 + self.c}

    def peer(self, d):
        df, dc = d // 2, d % 2
        core = 1 - self.c if dc else self.c
        return {"fsdp": self.flip(df), "expert": self.z * 2 + core}

    def flip(self, df):
        other, bit = 0, 1
        while bit < self.nf:
            digit = lax.rem(self.f // bit, 2)
            other = other + bit * (1 - digit if df & bit else digit)
            bit *= 2
        return other

    def greet(self):
        barrier = pltpu.get_barrier_semaphore()
        others = [self.plane(k) for k in range(1, self.nz)] + [self.peer(d) for d in range(1, 2 * self.nf)]
        for other in others:
            pl.semaphore_signal(barrier, inc=1, device_id=other, device_id_type=MESH)
        pl.semaphore_wait(barrier, len(others))


def remote(source, target, send, recv, device):
    return pltpu.make_async_remote_copy(
        src_ref=source, dst_ref=target, send_sem=send, recv_sem=recv, device_id=device, device_id_type=MESH
    )


def experts_kernel(
    nf, nz, cap, me_ref, place_ref, spot_ref, router_ref, block_ref, wg_any, wu_any, wd_any, *refs
):
    me = Place(nf, nz)
    near = 2 * nf
    early_refs, late_refs, refs = refs[:near], (None, *refs[near : near + nz - 1]), refs[near + nz - 1 :]
    own_ref, arrived_ref, blocks_ref, out_any, act_any, de_any, dgate_any, dup_any, back_ref, parts_ref, cots_ref = refs[:11]
    held, out, rows, cot, wg, wu, wd, de, act, dgate, dup, result, back, part, late, cot_out = refs[11:27]
    z_send, z_recv, sent, got, r_sent, r_got, p_send, p_recv, keep, loads, cot_loads, w_loads, stores, c_sent, c_got = refs[27:]
    width = rows.shape[1]
    tile = 256

    order = [*range(1, nz), 0]
    place_in = {k: i for i, k in enumerate(order)}

    def at(d):
        return pl.ds(d * cap, cap)

    def slot(k):
        return place_in[k] % 2

    def earlier(k, steps):
        return order[place_in[k] - steps] if place_in[k] >= steps else None

    def move(k):
        return remote(block_ref, held.at[k], z_send.at[k], z_recv.at[k], me.plane(k))

    def hop(k, d):
        there = arrived_ref.at[k, at(d)]
        if d == 0:
            return pltpu.make_async_copy(out.at[slot(k), at(d)], there, got.at[k, d])
        return remote(out.at[slot(k), at(d)], there, sent.at[k, d], got.at[k, d], me.peer(d))

    def hop_cot(k, d):
        there = cots_ref.at[k - 1, at(d)]
        if d == 0:
            return pltpu.make_async_copy(cot_out.at[slot(k), at(d)], there, c_got.at[k, d])
        return remote(cot_out.at[slot(k), at(d)], there, c_sent.at[k, d], c_got.at[k, d], me.peer(d))

    def load_cot(k):
        return pltpu.make_async_copy(late_refs[k], late, cot_loads.at[k, 0])

    def hop_back(k, d):
        there = back_ref.at[k, at(d)]
        if d == 0:
            return pltpu.make_async_copy(back.at[slot(k), at(d)], there, r_got.at[k, d])
        return remote(back.at[slot(k), at(d)], there, r_sent.at[k, d], r_got.at[k, d], me.peer(d))

    def along(k):
        return remote(
            part.at[k % 2], parts_ref.at[k - 1], p_send.at[k - 1], p_recv.at[k - 1], me.plane(nz - k)
        )

    def keep_block(k):
        return pltpu.make_async_copy(held.at[k], blocks_ref.at[k], keep.at[k])

    weights = [
        pltpu.make_async_copy(source.at[0], target, w_loads.at[i])
        for i, (source, target) in enumerate(((wg_any, wg), (wu_any, wu), (wd_any, wd)))
    ]
    own = pltpu.make_async_copy(block_ref, held.at[0], z_recv.at[0])

    def saves(k):
        pairs = ((result, out_any), (act, act_any), (de, de_any), (dgate, dgate_any), (dup, dup_any))
        return [pltpu.make_async_copy(source, target.at[k], stores.at[k, i]) for i, (source, target) in enumerate(pairs)]

    def gather(k):
        if k:
            move(k).wait_recv()
        else:
            own.wait()
        keep_block(k).start()
        if earlier(k, 2) is not None:
            for d in range(1, near):
                hop(earlier(k, 2), d).wait_send()
        for d in range(near):
            out[slot(k), at(d)] = jnp.dot(place_ref[k, d], held[k], preferred_element_type=jnp.float32).astype(
                jnp.bfloat16
            )
        for d in range(1, near):
            hop(k, d).start()
        hop(k, 0).start()

    def gather_cot(k):
        load_cot(k).wait()
        if k > 2:
            for d in range(1, near):
                hop_cot(k - 2, d).wait_send()
        for d in range(near):
            cot_out[slot(k), at(d)] = jnp.dot(place_ref[k, d], late[...], preferred_element_type=jnp.float32).astype(
                jnp.bfloat16
            )
        for d in range(1, near):
            hop_cot(k, d).start()
        hop_cot(k, 0).start()
        if k + 1 < nz:
            load_cot(k + 1).start()

    def expert(k):
        for d in range(near):
            hop(k, d).wait() if d == 0 else hop(k, d).wait_recv()
        load = pltpu.make_async_copy(arrived_ref.at[k], rows, loads.at[k])
        load.start()
        if k:
            for d in range(near):
                hop_cot(k, d).wait() if d == 0 else hop_cot(k, d).wait_recv()
            cot_moves = [
                pltpu.make_async_copy(cots_ref.at[k - 1], cot.at[:, pl.ds(0, late.shape[1])], cot_loads.at[k, 1])
            ]
        else:
            cot_moves = [
                pltpu.make_async_copy(early_refs[d], cot.at[at(d), pl.ds(0, late.shape[1])], cot_loads.at[0, d])
                for d in range(near)
            ]
        for one in cot_moves:
            one.start()
        if earlier(k, 1) is not None:
            for one in saves(earlier(k, 1)):
                one.wait()
        else:
            for one in weights:
                one.wait()
        load.wait()
        for one in cot_moves:
            one.wait()
        for d in range(near):
            span = at(d)
            logits = jnp.dot(rows[span, :], router_ref[...], preferred_element_type=jnp.float32)
            picked = cot[span, width : width + logits.shape[1]].astype(jnp.float32) > 0.5
            highest = jnp.max(jnp.where(picked, logits, NEG), axis=-1, keepdims=True)
            raised = jnp.exp(jnp.where(picked, logits - highest, NEG))
            lane = lax.broadcasted_iota(jnp.int32, logits.shape, 1)
            mine = jnp.sum(jnp.where(lane == me_ref[0], raised, 0.0), axis=-1, keepdims=True)
            gate = mine / jnp.maximum(jnp.sum(raised, axis=-1, keepdims=True), 1e-30)
            de[span, :] = (gate * cot[span, :width].astype(jnp.float32)).astype(jnp.bfloat16)

        def hidden(j, _):
            cols = pl.ds(pl.multiple_of(j * tile, tile), tile)
            gate_pre = jnp.dot(rows[...], wg[:, cols], preferred_element_type=jnp.float32)
            up_pre = jnp.dot(rows[...], wu[:, cols], preferred_element_type=jnp.float32)
            sigma = jax.nn.sigmoid(gate_pre)
            act[:, cols] = (gate_pre * sigma * up_pre).astype(jnp.bfloat16)
            d_act = right_product(de[...], wd[cols, :])
            dgate[:, cols] = (d_act * up_pre * sigma * (1.0 + gate_pre * (1.0 - sigma))).astype(jnp.bfloat16)
            dup[:, cols] = (d_act * gate_pre * sigma).astype(jnp.bfloat16)
            return 0

        lax.fori_loop(0, act.shape[1] // tile, hidden, 0)
        if earlier(k, 2) is not None:
            for d in range(1, near):
                hop_back(earlier(k, 2), d).wait_send()

        def model(n, rest):
            cols = pl.ds(pl.multiple_of(n * tile, tile), tile)
            result[:, cols] = jnp.dot(act[...], wd[:, cols], preferred_element_type=jnp.float32).astype(jnp.bfloat16)
            d_rows = right_product(dgate[...], wg[cols, :]) + right_product(dup[...], wu[cols, :])
            back[slot(k), :, cols] = d_rows.astype(jnp.bfloat16)
            return rest + jnp.sum(
                cot[:, cols].astype(jnp.float32) * result[:, cols].astype(jnp.float32), axis=-1, keepdims=True
            )

        rest = lax.fori_loop(0, width // tile, model, jnp.zeros((near * cap, 1), jnp.float32))
        shape = (near * cap, back.shape[2] - width)
        lane = lax.broadcasted_iota(jnp.int32, shape, 1) - (lax.broadcasted_iota(jnp.int32, shape, 0) // cap + k * near) * 3
        extra = jnp.zeros(shape, jnp.float32)
        for i in range(3):
            term = rest.astype(jnp.bfloat16).astype(jnp.float32)
            extra = jnp.where(lane == i, term, extra)
            rest = rest - term
        back[slot(k), :, width:] = extra.astype(jnp.bfloat16)
        for d in range(1, near):
            hop_back(k, d).start()
        hop_back(k, 0).start()
        for one in saves(k):
            one.start()

    def combine(k):
        for d in range(near):
            hop_back(k, d).wait() if d == 0 else hop_back(k, d).wait_recv()
        load = pltpu.make_async_copy(back_ref.at[k], cot.at[:, pl.ds(0, back.shape[2])], loads.at[nz + k])
        load.start()
        load.wait()
        for d in range(near):
            term = jnp.dot(spot_ref[k, d], cot[at(d), : back.shape[2]], preferred_element_type=jnp.float32)
            if d:
                own_ref[...] += term
            else:
                own_ref[...] = term
        if k:
            if k > 2:
                along(k - 2).wait_send()
            part[k % 2] = own_ref[...].astype(jnp.bfloat16)
            along(k).start()

    for one in weights:
        one.start()
    me.greet()
    for k in range(1, nz):
        move(k).start()
    own.start()
    load_cot(1).start()
    gather_cot(1)
    gather(1)
    for k in range(1, nz):
        if k + 1 < nz:
            gather_cot(k + 1)
        if k == 1:
            expert(k)
        if k + 1 < nz:
            gather(k + 1)
        else:
            gather(0)
        if k > 1:
            combine(k - 1)
            expert(k)
    combine(nz - 1)
    expert(0)
    combine(0)
    for k in range(nz):
        keep_block(k).wait()
        if k:
            move(k).wait_send()
            if k >= nz - 2:
                along(k).wait_send()
            along(k).wait_recv()
    for k in order[-2:]:
        for d in range(1, near):
            hop(k, d).wait_send()
            hop_back(k, d).wait_send()
    for k in (nz - 2, nz - 1):
        for d in range(1, near):
            hop_cot(k, d).wait_send()
    for one in saves(order[-1]):
        one.wait()


def run_experts(nf, me, place, spot, router, block, w_gate, w_up, w_down, early, late):
    nz, near, cap, count = place.shape
    width, hidden = w_gate.shape[1:]
    rows = near * cap
    extra = -(-3 * near * nz // 128) * 128
    wide = max(width + extra, early[0].shape[1])
    low = jnp.bfloat16
    anywhere = pl.BlockSpec(memory_space=pl.ANY)
    own = jax.ShapeDtypeStruct((count, width + extra), jnp.float32)
    shapes = [
        jax.ShapeDtypeStruct(shape, low)
        for shape in (
            (nz, rows, width),
            (nz, count, width),
            (nz, rows, width),
            (nz, rows, hidden),
            (nz, rows, width),
            (nz, rows, hidden),
            (nz, rows, hidden),
            (nz, rows, width + extra),
            (nz - 1, count, width + extra),
            (nz - 1, rows, early[0].shape[1]),
        )
    ]
    dma = pltpu.SemaphoreType.DMA
    return pl.pallas_call(
        lambda *refs: experts_kernel(nf, nz, cap, *refs),
        in_specs=[SCALARS, whole_spec(place), whole_spec(spot), whole_spec(router)] + [anywhere] * (4 + near + len(late)),
        out_specs=[whole_spec(own)] + [anywhere] * len(shapes),
        out_shape=[own] + shapes,
        scratch_shapes=[
            pltpu.VMEM((nz, count, width), low),
            pltpu.VMEM((2, rows, width), low),
            pltpu.VMEM((rows, width), low),
            pltpu.VMEM((rows, wide), low),
            pltpu.VMEM((width, hidden), low),
            pltpu.VMEM((width, hidden), low),
            pltpu.VMEM((hidden, width), low),
            pltpu.VMEM((rows, width), low),
            pltpu.VMEM((rows, hidden), low),
            pltpu.VMEM((rows, hidden), low),
            pltpu.VMEM((rows, hidden), low),
            pltpu.VMEM((rows, width), low),
            pltpu.VMEM((2, rows, width + extra), low),
            pltpu.VMEM((2, count, width + extra), low),
            pltpu.VMEM((count, early[0].shape[1]), low),
            pltpu.VMEM((2, rows, early[0].shape[1]), low),
            dma((nz,)),
            dma((nz,)),
            dma((nz, near)),
            dma((nz, near)),
            dma((nz, near)),
            dma((nz, near)),
            dma((nz - 1,)),
            dma((nz - 1,)),
            dma((nz,)),
            dma((2 * nz,)),
            dma((nz, near)),
            dma((3,)),
            dma((nz, 5)),
            dma((nz, near)),
            dma((nz, near)),
        ],
        compiler_params=pltpu.CompilerParams(collective_id=0, has_side_effects=True, vmem_limit_bytes=MOST_VMEM),
        cost_estimate=pl.CostEstimate(
            flops=12 * nz * rows * width * hidden, bytes_accessed=600_000_000, transcendentals=0
        ),
        name="run_experts",
    )(me, place, spot, router, block, w_gate, w_up, w_down, *early, *late)


def whole_spec(value):
    return pl.BlockSpec(value.shape, lambda *_: (0,) * len(value.shape))


SCALARS = pl.BlockSpec(memory_space=pltpu.SMEM)


def scores_of(q_rot, k_rot, seg_col, seg_row):
    scores = right_product(q_rot, k_rot) * HEAD_SIZE ** (-0.5)
    here = lax.broadcasted_iota(jnp.int32, scores.shape, 0) >= lax.broadcasted_iota(jnp.int32, scores.shape, 1)
    return jnp.where(here & (seg_col == seg_row), scores, NEG)


def turn(value, cos, sin):
    return value * cos + pltpu.roll(value, HEAD_SIZE // 2, 1) * sin


def attend_kernel(blocks, heads, kv_heads, spots, x_ref, gain_ref, row_ref, col_ref, cos_ref, sin_ref, qg_ref, kg_ref, *refs):
    w_refs, refs = refs[:blocks], refs[blocks:]
    normed_ref, raw_ref, rot_ref, value_ref, mixed_ref, lse_ref = refs
    wide = x_ref[...].astype(jnp.float32)
    normed_ref[...] = (wide * inverse_norm(wide) * gain_ref[...]).astype(jnp.bfloat16)
    depth = w_refs[0].shape[0]
    total = None
    for i, w_ref in enumerate(w_refs):
        part = normed_ref[...] if blocks == 1 else normed_ref[:, pl.ds(pl.multiple_of(spots[i] * depth, depth), depth)]
        part = jnp.dot(part, w_ref[...], preferred_element_type=jnp.float32)
        total = part if total is None else total + part
    turned = (heads + kv_heads) * HEAD_SIZE
    raw_ref[...] = total[:, :turned]
    value_ref[...] = total[:, turned:].astype(jnp.bfloat16)
    cos, sin = cos_ref[...], sin_ref[...]
    for h in range(heads + kv_heads):
        at = slice(h * HEAD_SIZE, (h + 1) * HEAD_SIZE)
        raw = raw_ref[:, at]
        gain = qg_ref[...] if h < heads else kg_ref[...]
        rot_ref[:, at] = turn(raw * inverse_norm(raw) * gain, cos, sin).astype(jnp.bfloat16)
    lane = lax.broadcasted_iota(jnp.int32, lse_ref.shape, 1)
    all_lse = jnp.zeros(lse_ref.shape, jnp.float32)
    for h in range(heads):
        at = slice(h * HEAD_SIZE, (h + 1) * HEAD_SIZE)
        g = h * kv_heads // heads
        masked = scores_of(
            rot_ref[:, at],
            rot_ref[:, (heads + g) * HEAD_SIZE : (heads + g + 1) * HEAD_SIZE],
            col_ref[...],
            row_ref[...],
        )
        top = jnp.max(masked, axis=-1, keepdims=True)
        lse = top + jnp.log(jnp.sum(jnp.exp(masked - top), axis=-1, keepdims=True))
        prob_low = jnp.exp(masked - lse).astype(jnp.bfloat16)
        mixed_ref[:, at] = jnp.dot(
            prob_low, value_ref[:, g * HEAD_SIZE : (g + 1) * HEAD_SIZE], preferred_element_type=jnp.float32
        ).astype(jnp.bfloat16)
        all_lse = jnp.where(lane == h, lse, all_lse)
    lse_ref[...] = all_lse


def attend(spots, tokens, gain, seg_row, seg_col, cos, sin, qg, kg, w_blocks, heads, kv_heads):
    count, width = tokens.shape
    args = (tokens, gain, seg_row, seg_col, cos, sin, qg, kg, *w_blocks)
    shapes = [
        jax.ShapeDtypeStruct((count, width), jnp.bfloat16),
        jax.ShapeDtypeStruct((count, (heads + kv_heads) * HEAD_SIZE), jnp.float32),
        jax.ShapeDtypeStruct((count, (heads + kv_heads) * HEAD_SIZE), jnp.bfloat16),
        jax.ShapeDtypeStruct((count, kv_heads * HEAD_SIZE), jnp.bfloat16),
        jax.ShapeDtypeStruct((count, heads * HEAD_SIZE), jnp.bfloat16),
        jax.ShapeDtypeStruct((count, 128), jnp.float32),
    ]
    return pl.pallas_call(
        lambda *refs: attend_kernel(len(w_blocks), heads, kv_heads, *refs),
        in_specs=[SCALARS] + [whole_spec(v) for v in args],
        out_specs=[whole_spec(v) for v in shapes],
        out_shape=shapes,
        cost_estimate=pl.CostEstimate(
            flops=2 * count * width * (heads + 2 * kv_heads) * HEAD_SIZE + 4 * heads * count * count * HEAD_SIZE,
            bytes_accessed=2 * width * (heads + 2 * kv_heads) * HEAD_SIZE + 16 * count * width,
            transcendentals=2 * heads * count * count,
        ),
        name="attend",
    )(spots, *args)


def project_kernel(blocks, spots, mixed_ref, *refs):
    w_refs, out_ref = refs[:blocks], refs[-1]
    depth = w_refs[0].shape[0]
    total = None
    for i, w_ref in enumerate(w_refs):
        part = mixed_ref[...] if blocks == 1 else mixed_ref[:, pl.ds(pl.multiple_of(spots[i] * depth, depth), depth)]
        part = jnp.dot(part, w_ref[...], preferred_element_type=jnp.float32)
        total = part if total is None else total + part
    out_ref[...] = total.astype(out_ref.dtype)


def project(spots, mixed, w_blocks, dtype):
    count, depth = mixed.shape
    width = w_blocks[0].shape[1]
    return pl.pallas_call(
        lambda *refs: project_kernel(len(w_blocks), *refs),
        grid=(width // WIDE,),
        in_specs=[SCALARS, pl.BlockSpec((count, depth), lambda j: (0, 0))]
        + [pl.BlockSpec((w.shape[0], WIDE), lambda j: (0, j)) for w in w_blocks],
        out_specs=pl.BlockSpec((count, WIDE), lambda j: (0, j)),
        out_shape=jax.ShapeDtypeStruct((count, width), dtype),
        cost_estimate=pl.CostEstimate(
            flops=2 * count * depth * width, bytes_accessed=2 * depth * width + 4 * count * width, transcendentals=0
        ),
        name="project",
    )(spots, mixed, *w_blocks)


def head_back(grad_rot, raw, gain, cos, sin):
    grad_normed = turn(grad_rot, cos, -sin)
    rinv = inverse_norm(raw)
    gain_grad = jnp.sum(grad_normed * raw * rinv, axis=0, keepdims=True)
    scaled = grad_normed * gain
    return rinv * scaled - raw * rinv**3 * jnp.mean(scaled * raw, axis=-1, keepdims=True), gain_grad


def attend_back_kernel(
    blocks, heads, kv_heads, spots, dmid_ref, x_ref, row_ref, col_ref, cos_ref, sin_ref, qg_ref, kg_ref,
    raw_ref, rot_ref, value_ref, mixed_ref, lse_ref, *refs
):
    o_refs, w_refs, refs = refs[:blocks], refs[blocks : 2 * blocks], refs[2 * blocks :]
    dheads_ref, part_ref, gain_ref, qgain_ref, kgain_ref, dmixed = refs
    scale = HEAD_SIZE ** (-0.5)
    dmid = dmid_ref[...]
    depth = o_refs[0].shape[0]
    for i, o_ref in enumerate(o_refs):
        part = right_product(dmid, o_ref[...]).astype(jnp.bfloat16)
        if blocks == 1:
            dmixed[...] = part
        else:
            dmixed[:, pl.ds(pl.multiple_of(spots[i] * depth, depth), depth)] = part
    cos, sin = cos_ref[...], sin_ref[...]
    lane = lax.broadcasted_iota(jnp.int32, lse_ref.shape, 1)
    all_lse = lse_ref[...]
    q_gain = jnp.zeros(qgain_ref.shape, jnp.float32)
    k_gain = jnp.zeros(kgain_ref.shape, jnp.float32)
    for g in range(kv_heads):
        kv = slice(g * HEAD_SIZE, (g + 1) * HEAD_SIZE)
        key_at = slice((heads + g) * HEAD_SIZE, (heads + g + 1) * HEAD_SIZE)
        k_rot, value = rot_ref[:, key_at], value_ref[:, kv]
        d_value, d_key = None, None
        for h in range(g * heads // kv_heads, (g + 1) * heads // kv_heads):
            at = slice(h * HEAD_SIZE, (h + 1) * HEAD_SIZE)
            q_rot, grad = rot_ref[:, at], dmixed[:, at]
            lse = jnp.sum(jnp.where(lane == h, all_lse, 0.0), axis=-1, keepdims=True)
            prob = jnp.exp(scores_of(q_rot, k_rot, col_ref[...], row_ref[...]) - lse)
            part = left_product(prob.astype(jnp.bfloat16), grad)
            d_value = part if d_value is None else d_value + part
            d_prob = right_product(grad, value)
            delta = jnp.sum(grad.astype(jnp.float32) * mixed_ref[:, at].astype(jnp.float32), axis=-1, keepdims=True)
            d_scores = (prob * (d_prob - delta)).astype(jnp.bfloat16)
            part = left_product(d_scores, q_rot)
            d_key = part if d_key is None else d_key + part
            d_q = jnp.dot(d_scores, k_rot, preferred_element_type=jnp.float32) * scale
            d_query, gain_part = head_back(d_q, raw_ref[:, at], qg_ref[...], cos, sin)
            q_gain = q_gain + gain_part
            dheads_ref[:, at] = d_query.astype(jnp.bfloat16)
        d_key, gain_part = head_back(d_key * scale, raw_ref[:, key_at], kg_ref[...], cos, sin)
        k_gain = k_gain + gain_part
        dheads_ref[:, key_at] = d_key.astype(jnp.bfloat16)
        last = (heads + kv_heads + g) * HEAD_SIZE
        dheads_ref[:, last : last + HEAD_SIZE] = d_value.astype(jnp.bfloat16)
    qgain_ref[...] = q_gain
    kgain_ref[...] = k_gain
    d_heads = dheads_ref[...]
    wide = x_ref[...].astype(jnp.float32)
    rinv = inverse_norm(wide)
    depth = w_refs[0].shape[0]
    for i, w_ref in enumerate(w_refs):
        part = right_product(d_heads, w_ref[...])
        at = slice(None) if blocks == 1 else pl.ds(pl.multiple_of(spots[i] * depth, depth), depth)
        part_ref[:, at] = part.astype(part_ref.dtype)
        x = x_ref[:, at].astype(jnp.float32)
        gain_ref[:, at] = jnp.sum(part * x * rinv, axis=0, keepdims=True)


def attend_back(spots, dmid, tokens, seg_row, seg_col, cos, sin, qg, kg, saved, o_blocks, w_blocks, heads, kv_heads, dtype):
    count, width = tokens.shape
    args = (dmid, tokens, seg_row, seg_col, cos, sin, qg, kg, *saved, *o_blocks, *w_blocks)
    lanes = (heads + 2 * kv_heads) * HEAD_SIZE
    shapes = [
        jax.ShapeDtypeStruct((count, lanes), jnp.bfloat16),
        jax.ShapeDtypeStruct((count, width), dtype),
        jax.ShapeDtypeStruct((1, width), jnp.float32),
        jax.ShapeDtypeStruct((1, HEAD_SIZE), jnp.float32),
        jax.ShapeDtypeStruct((1, HEAD_SIZE), jnp.float32),
    ]
    return pl.pallas_call(
        lambda *refs: attend_back_kernel(len(w_blocks), heads, kv_heads, *refs),
        in_specs=[SCALARS] + [whole_spec(v) for v in args],
        out_specs=[whole_spec(v) for v in shapes],
        out_shape=shapes,
        scratch_shapes=[pltpu.VMEM((count, heads * HEAD_SIZE), jnp.bfloat16)],
        cost_estimate=pl.CostEstimate(
            flops=4 * count * width * lanes + 10 * heads * count * count * HEAD_SIZE,
            bytes_accessed=4 * width * lanes + 24 * count * width,
            transcendentals=heads * count * count,
        ),
        name="attend_back",
    )(spots, *args)


def on_device(
    tokens,
    segments,
    routes,
    attn_gain,
    w_query,
    key_matrix,
    value_matrix,
    output_matrix,
    query_gain,
    key_gain,
    ffn_gain,
    w_router,
    w_gate,
    w_up,
    w_down,
    cotangent,
):
    nf, ne = lax.axis_size("fsdp"), lax.axis_size("expert")
    nz = ne // 2
    f, e = lax.axis_index("fsdp"), lax.axis_index("expert")
    z, c = e // 2, e % 2
    count = tokens.shape[0]
    experts = nf * ne
    cap = -(5 * count * TOP // (4 * experts)) // 16 * -16
    peers = [(df, dc) for df in range(nf) for dc in range(2)]
    near = len(peers)

    def across(value, df, dc):
        return lax.ppermute(
            value, ALL, [(i * ne + j, (i ^ df) * ne + (j ^ dc)) for i in range(nf) for j in range(ne)]
        )

    def along(value, k):
        return lax.ppermute(value, "expert", [(j, (j + 2 * k) % ne) for j in range(ne)])

    def group_blocks(value):
        return [value] + [across(value, df, 0) for df in range(1, nf)]

    def plane_blocks(value):
        blocks = [value]
        for k in range(1, nz):
            blocks.append(along(value, k))
        return blocks

    def spread_rows(blocks):
        rows, width = blocks[0].shape
        places, pieces = [], []
        for k, block in enumerate(blocks):
            places += [(z - k) % nz * 2 + c, (z - k) % nz * 2 + 1 - c]
            pieces += [block, across(block, 0, 1)]
        if rows % 128 == 0:
            return pieces, jnp.stack(places).astype(jnp.int32)
        whole = jnp.zeros((ne, rows, width), blocks[0].dtype)
        for at, piece in zip(places, pieces):
            whole = lax.dynamic_update_slice(whole, piece[None], (at, 0, 0))
        return [whole.reshape(ne * rows, width)], jnp.zeros((1,), jnp.int32)

    def reduce_rows(grad):
        grad = grad.reshape(nz, 2, grad.shape[0] // ne, grad.shape[1])
        theirs = lax.dynamic_index_in_dim(grad, 1 - c, 1, keepdims=False).astype(jnp.bfloat16)
        mine = lax.dynamic_index_in_dim(grad, c, 1, keepdims=False)
        mine = mine + across(theirs, 0, 1).astype(jnp.float32)
        total = lax.dynamic_index_in_dim(mine, z, 0, keepdims=False)
        parts = [lax.dynamic_index_in_dim(mine, (z + k) % nz, 0, keepdims=False) for k in range(1, nz)]
        parts = [part.astype(jnp.bfloat16) for part in parts]
        for k, part in enumerate(parts, 1):
            total = total + along(part, k).astype(jnp.float32)
        return total, parts

    def add_pairs(values):
        while len(values) > 1:
            values = [a + b for a, b in zip(values[::2], values[1::2])]
        return values[0]

    def sum_small(lines, row):
        own = MODEL_WIDTH // ne
        blocks = jnp.transpose(lines.reshape(lines.shape[0], nz, 2, own), (1, 2, 0, 3))
        rows = row.reshape(row.size // own, own)
        rows = jnp.pad(rows, ((0, -(rows.shape[0] + lines.shape[0]) % 8), (0, 0)))
        blocks = jnp.concatenate([blocks, jnp.broadcast_to(rows[None, None], (nz, 2) + rows.shape)], axis=2)
        mine = lax.dynamic_index_in_dim(blocks, c, 1, keepdims=False)
        mine = mine + across(lax.dynamic_index_in_dim(blocks, 1 - c, 1, keepdims=False), 0, 1)
        got = [lax.dynamic_index_in_dim(mine, z, 0, keepdims=False)]
        for step in range(1, nz):
            part = lax.dynamic_index_in_dim(mine, z ^ step, 0, keepdims=False)
            got.append(lax.ppermute(part, "expert", [(j, j ^ (2 * step)) for j in range(ne)]))
        return add_pairs(got)

    width_q, width_k = w_query.shape[1], key_matrix.shape[1]
    w_heads = jnp.concatenate([w_query, key_matrix, value_matrix], axis=1)
    token_blocks = group_blocks(tokens)
    segment_blocks = group_blocks(segments)
    few = jnp.concatenate(
        [jnp.transpose(routes).astype(jnp.bfloat16).reshape(-1, w_router.shape[0]), attn_gain[None], ffn_gain[None], jnp.transpose(w_router)]
    )
    few_blocks = plane_blocks(few)
    heads_blocks = plane_blocks(after(w_heads, few))
    few_pairs = across(jnp.stack([block[-experts - 2 :] for block in few_blocks]), 0, 1)
    few_whole = jnp.zeros((nz, 2) + few_pairs.shape[1:], jnp.bfloat16)
    for k, block in enumerate(few_blocks):
        for core, piece in ((c, block[-experts - 2 :]), (1 - c, few_pairs[k])):
            few_whole = lax.dynamic_update_slice(few_whole, piece[None, None], ((z - k) % nz, core, 0, 0))
    few_whole = jnp.transpose(few_whole, (2, 0, 1, 3)).reshape(experts + 2, MODEL_WIDTH)
    gain_one, gain_two = few_whole[:1].astype(jnp.float32), few_whole[1:2].astype(jnp.float32)
    full_router = jnp.transpose(jnp.pad(few_whole[2:], ((0, -experts % 128), (0, 0))))
    route_blocks = [block[: -experts - 2].reshape(TOP, count).astype(jnp.int32) for block in few_blocks]
    picked = jnp.any(routes[:, :, None] == jnp.arange(full_router.shape[1])[None, None, :], axis=1)
    cot_wide = jnp.concatenate([cotangent, picked.astype(jnp.bfloat16)], axis=1)

    peer_experts = jnp.stack([(f ^ df) * ne + 2 * z + (c ^ dc) for df, dc in peers])
    named = jnp.stack(route_blocks)
    hit = jnp.any(named[:, None] == peer_experts[None, :, None, None], axis=2)
    upto = (jnp.arange(count)[:, None] <= jnp.arange(count)[None, :]).astype(jnp.bfloat16)
    rank = jnp.dot(
        hit.astype(jnp.bfloat16).reshape(nz * near, count), upto, preferred_element_type=jnp.float32
    ).reshape(nz, near, count)
    slot_of = jnp.where(hit, rank - 1.0, -1.0)
    slots = jnp.arange(cap, dtype=jnp.float32)
    place = (slot_of[:, :, None, :] == slots[None, None, :, None]).astype(jnp.bfloat16)
    spot = (slot_of[:, :, :, None] == slots[None, None, None, :]).astype(jnp.bfloat16)

    def send_out(pieces):
        got = [pieces[0]]
        for d, (df, dc) in enumerate(peers[1:], 1):
            got.append(across(pieces[d], df, dc))
        return got

    early = send_out(gather_slots(place, (0,), [after(cot_wide, *token_blocks[1:])]))

    local_q = width_q // HEAD_SIZE
    local_kv = width_k // HEAD_SIZE
    w_blocks, spots = spread_rows([after(block, few_whole) for block in heads_blocks])
    head_blocks = plane_blocks(after(output_matrix, *w_blocks))
    cot_blocks = plane_blocks(after(cot_wide, *w_blocks))
    cosine, sine = rotary_tables(SEQ, HEAD_SIZE)
    cos = jnp.concatenate([cosine[0, :, 0], cosine[0, :, 0]], axis=-1)
    sin = jnp.concatenate([-sine[0, :, 0], sine[0, :, 0]], axis=-1)
    q_scale = query_gain.astype(jnp.float32)[None]
    k_scale = key_gain.astype(jnp.float32)[None]
    turns = [1 + df for df in range(nf - 1)] + [0]
    shared = [
        (segment_blocks[df], jnp.transpose(segment_blocks[df]), cos, sin, q_scale, k_scale) for df in range(nf)
    ]
    attended = [None] * nf
    for turn_at, df in enumerate(turns):
        attended[df] = attend(
            spots,
            after(token_blocks[df], *([attended[turns[turn_at - 1]][4]] if turn_at else [])),
            gain_one,
            *shared[df],
            w_blocks,
            local_q,
            local_kv,
        )
    o_blocks, _ = spread_rows([after(block, attended[turns[-2]][0]) for block in head_blocks])
    wide_in = tokens.astype(jnp.float32)
    rinv_one = inverse_norm(wide_in)
    residual_mid = wide_in
    for df in turns:
        part = project(spots, attended[df][4], o_blocks, jnp.bfloat16 if df else jnp.float32)
        if df:
            part = across(part, df, 0).astype(jnp.float32)
        residual_mid = residual_mid + part

    rinv_two = inverse_norm(residual_mid)
    normed_two = (residual_mid * rinv_two * gain_two).astype(jnp.bfloat16)
    me = (f * ne + e).astype(jnp.int32)[None]
    own_sum, arrived, normed_blocks, expert_out, act, d_expert, d_gate_pre, d_up_pre, _, plane_sums, _ = run_experts(
        nf, me, place, spot, full_router, normed_two, w_gate, w_up, w_down, early, cot_blocks[1:]
    )
    back_sum = own_sum + jnp.sum(plane_sums.astype(jnp.float32), axis=0)
    d_normed_two = back_sum[:, :MODEL_WIDTH]

    def gates_of(rows, named_rows):
        logits = jnp.dot(rows, full_router, preferred_element_type=jnp.float32)[:, :experts]
        picked = jnp.any(named_rows[:, :, None] == jnp.arange(experts)[None, None, :], axis=0)
        highest = jnp.max(jnp.where(picked, logits, NEG), axis=-1, keepdims=True)
        raised = jnp.where(picked, jnp.exp(jnp.minimum(logits - highest, 0.0)), 0.0)
        return raised / jnp.sum(raised, axis=-1, keepdims=True)

    gates = gates_of(normed_two, route_blocks[0])

    owners = jnp.concatenate(
        [jnp.repeat(peer_experts + 2 * ((z + k) % nz - z), 3) for k in range(nz)]
    )
    names = (owners[:, None] == jnp.arange(experts)[None, :]).astype(jnp.float32)
    d_gates = jnp.dot(
        back_sum[:, MODEL_WIDTH : MODEL_WIDTH + 3 * near * nz], names, precision=lax.Precision.HIGHEST
    )
    d_logits = (gates * (d_gates - jnp.sum(gates * d_gates, axis=-1, keepdims=True))).astype(jnp.bfloat16)

    router_grad = left_product(d_logits, normed_two)[:experts]
    d_normed_two = d_normed_two + right_product(d_logits, full_router[:, :experts])
    d_norm_part, gain_two_grad = row_norm_back(d_normed_two, residual_mid, rinv_two, gain_two)
    d_mid = cotangent.astype(jnp.float32) + d_norm_part
    middle_blocks = group_blocks(d_mid.astype(jnp.bfloat16))
    arrived, act, d_expert, d_gate_pre, d_up_pre = after(
        tuple(
            value.reshape(nz * near * cap, value.shape[2])
            for value in (arrived, act, d_expert, d_gate_pre, d_up_pre)
        ),
        middle_blocks[0],
    )
    down_grad = left_product(act, d_expert)
    gate_grad = left_product(arrived, d_gate_pre)
    up_grad = left_product(arrived, d_up_pre)

    is_peer = peer_experts[None, :, None] == jnp.arange(experts)[None, None, :]
    peer_gates = jnp.stack(
        [
            jnp.sum(jnp.where(is_peer, gates_of(normed_blocks[k], route_blocks[k])[:, None, :], 0.0), axis=-1)
            for k in range(nz)
        ]
    )
    expert_out = after(expert_out, *middle_blocks[1:])
    groups = [list(range(1, nz // 2 + 1)), list(range(nz // 2 + 1, nz)) + [0]]
    come = {}
    for group in groups:
        pieces = [
            jnp.concatenate([expert_out[k, d * cap : (d + 1) * cap] for k in group], axis=0) for d in range(near)
        ]
        pieces = send_out(pieces)
        for i, k in enumerate(group):
            come[k] = (i, pieces)

    home_parts = {}

    def home_sum(k, weights):
        part = combine_slots(spot, k, *come[k], jnp.bfloat16 if k else jnp.float32, weights)
        home_parts[k] = part
        if k:
            part = along(part, nz - k).astype(jnp.float32)
        return part

    mixed = jnp.concatenate([attended[df][4] for df in range(nf)], axis=0)
    share_out, out_parts = reduce_rows(left_product(mixed, jnp.concatenate(middle_blocks, axis=0)))
    moe = [home_sum(k, after(peer_gates, *out_parts)) for k in groups[0]]
    d_heads = [None] * nf
    d_normed_one, gain_one_grad, q_gain_grad, k_gain_grad = None, None, None, None
    for df in range(nf):
        d_heads[df], part, *sums = attend_back(
            spots,
            after(
                middle_blocks[df],
                *([d_heads[df - 1]] if df else []),
                *([home_parts[k] for k in groups[0]] if df == nf - 1 else []),
            ),
            token_blocks[df],
            *shared[df],
            attended[df][1:],
            o_blocks,
            w_blocks,
            local_q,
            local_kv,
            jnp.bfloat16 if df else jnp.float32,
        )
        if df:
            part = across(part, df, 0).astype(jnp.float32)
            d_normed_one = d_normed_one + part
            gain_one_grad, q_gain_grad, k_gain_grad = [
                a + b for a, b in zip((gain_one_grad, q_gain_grad, k_gain_grad), sums)
            ]
        else:
            d_normed_one = part
            gain_one_grad, q_gain_grad, k_gain_grad = sums
    normed_one = jnp.concatenate([attended[df][0] for df in range(nf)], axis=0)
    share_heads, head_parts = reduce_rows(left_product(normed_one, jnp.concatenate(d_heads, axis=0)))
    lines = jnp.concatenate([router_grad, gain_one_grad, gain_two_grad[None]], axis=0)
    small = sum_small(lines, jnp.concatenate([q_gain_grad, k_gain_grad], axis=1))
    for k in groups[1]:
        moe.append(home_sum(k, after(peer_gates, *head_parts)))
    moe = sum(moe[1:], moe[0])
    output = (residual_mid + moe).astype(jnp.bfloat16)
    small = after(small, home_parts[0])
    small = add_pairs([across(small, df, 0) if df else small for df in range(nf)])

    d_tokens, _ = row_norm_back(d_normed_one, wide_in, rinv_one, gain_one)
    token_grad = d_mid + d_tokens

    head_gains = small[experts + 2 :].reshape(-1)
    return (
        output,
        token_grad,
        small[experts],
        share_heads[:, :width_q],
        share_heads[:, width_q : width_q + width_k],
        share_heads[:, width_q + width_k :],
        share_out,
        head_gains[:HEAD_SIZE],
        head_gains[HEAD_SIZE : 2 * HEAD_SIZE],
        small[experts + 1],
        jnp.transpose(small[:experts]),
        gate_grad[None],
        up_grad[None],
        down_grad[None],
    )


def solution(mesh):
    return jax.shard_map(
        on_device,
        mesh=mesh,
        in_specs=(
            P(("fsdp", "expert"), None),
            P(("fsdp", "expert"), None),
            P(("fsdp", "expert"), None),
            P("expert"),
            P("expert", "fsdp"),
            P("expert", "fsdp"),
            P("expert", "fsdp"),
            P(("fsdp", "expert"), None),
            P(),
            P(),
            P("expert"),
            P("expert", None),
            P(("fsdp", "expert"), None, None),
            P(("fsdp", "expert"), None, None),
            P(("fsdp", "expert"), None, None),
            P(("fsdp", "expert"), None),
        ),
        out_specs=(
            P(("fsdp", "expert"), None),
            P(("fsdp", "expert"), None),
            P("expert"),
            P("expert", "fsdp"),
            P("expert", "fsdp"),
            P("expert", "fsdp"),
            P(("fsdp", "expert"), None),
            P(),
            P(),
            P("expert"),
            P("expert", None),
            P(("fsdp", "expert"), None, None),
            P(("fsdp", "expert"), None, None),
            P(("fsdp", "expert"), None, None),
        ),
        check_vma=False,
    )
```
